128 devices in a mesh: row: 8 (over z, core), col: 16 (over y, x).
Axes of the slice: x: 4, y: 4, z: 4, core: 2. Of those that a mesh axis runs over, the one named last changes fastest.
Arguments:
- ainv_anc: bfloat16 [24576, 24576], P('row', 'col'), may hold values from -6 to 6
- l_panel: bfloat16 [1536, 24576], P('col', 'row'), may hold values from -0.078125 to 0.078125
- diag_inv: float32 [1536, 768], P('col', 'row'), may hold values from -6 to 6
- struct_mask: int32 [2, 192], replicated, may hold values 0 or 1
- pieces: float32 [24576, 32, 128], P(('row', 'col')), may hold values from -6 to 6
- tile_owner: int32 [24576, 1], P(('row', 'col')), may hold values from 0 to 127; in each aligned block of 192 rows (0 to 191, 192 to 383, ...) at most 3 rows name the same one
Outputs:
- ainv_upper: bfloat16 [1536, 24576], P('col', 'row')
- ainv_diag: float32 [1536, 768], P('col', 'row')
- moved: float32 [49152, 32, 128], P(('row', 'col'))
The draws below stay inside these ranges and needn't reach their ends.
Inputs may be any that keep to these rules, and one draw needn't show every extreme that they name: `tile_owner`: among the 192 pieces of one device no owner is named more than 3 times, a bound that some block reaches.
All inputs are finite; a program needn't handle non-finite values.
Results may differ from the reference program's by a relative error of at most 0.015.
Values may be sent and summed in bfloat16 or wider, within the bound.
A program may use at most 128 MiB of HBM per device.

```python
import math
import jax
import jax.numpy as jnp
import numpy as np
from jax import lax

W = 768
NS = 2
AB = 128
SLOT = 3
TR = 32
TC = 128
ORDER = 24576
PANEL = 1536
NBLK = 192
TPD = 192
PIECES = 24576
N_ROW = 8
N_COL = 16
DEVICES = 128


def touch_ends(values, key, least, top_value):
    dims = values.shape
    index_at = [jax.random.randint(jax.random.fold_in(key, axis), (), 0, dims[axis]) for axis in range(len(dims))]
    values = values.at[tuple(index_at)].set(least)
    longest = dims.index(max(dims))
    index_at[longest] = (index_at[longest] + 1) % dims[longest]
    return values.at[tuple(index_at)].set(top_value)


def raised(values, own_key, source, target, parts, factor):
    def block_of(position):
        return (jnp.arange(values.shape[position]) // (values.shape[position] // parts)).reshape((-1,) + (1,) * (values.ndim - 1 - position))

    one_side = jax.random.permutation(own_key, parts)[block_of(target)]
    second = (block_of(target) + parts // 2) % parts
    return jnp.where((block_of(source) == one_side) | (block_of(source) == second), factor * values, values)


def shard_levels(key, extent, cuts, smallest, top_value):
    def one(position, parts):
        heights = jax.random.uniform(jax.random.fold_in(jax.random.fold_in(key, 6), position), (parts,), jnp.float32, smallest / len(cuts), top_value / len(cuts))
        return jnp.repeat(jnp.exp(heights), extent[position] // parts).reshape((-1,) + (1,) * (len(extent) - position - 1))

    loudness = one(*cuts[0])
    for cut in cuts[1:]:
        loudness = loudness * one(*cut)
    return loudness


def shared_out(key, own, number, rows, count, top, bound, skew):
    sequence = jax.random.permutation(key, count)
    crowded, common = load_shares(count, rows * top, bound, skew, True), load_shares(count, rows * top, bound, skew, False)
    places = jnp.arange(count)

    def named(tallies, offset_by):
        used = int((tallies > 0).sum())
        fixed = max(1, used // 4)
        passed = fixed + (places - fixed + offset_by * (used - fixed)) % max(1, count - fixed)
        return jnp.zeros((count,), jnp.int32).at[sequence[jnp.where(places < fixed, places, passed)]].set(jnp.asarray(tallies, jnp.int32))

    tallies = jnp.where(number % 4 == 0, named(crowded, number // 4), named(common, number - number // 4 - 1))
    mixed = jax.random.permutation(jax.random.fold_in(own, 3), count)
    donor, receiver = mixed[0:count // 2 * 2:2], mixed[1:count // 2 * 2:2]
    slack = jnp.minimum(tallies[donor] - 1, bound - tallies[receiver]) // 2
    slack = jnp.where((donor == sequence[0]) | (receiver == sequence[0]) | (tallies[receiver] == 0), 0, jnp.maximum(slack, 0))
    passed = jax.random.randint(jax.random.fold_in(own, 4), (count // 2,), 0, 1 << 20) % (slack + 1)
    tallies = tallies.at[donor].add(-passed).at[receiver].add(passed)
    members = jnp.searchsorted(jnp.cumsum(tallies), jnp.arange(rows * top), side="right").astype(jnp.int32)
    listing = members.reshape(top, rows).T
    listing = listing[jax.random.permutation(jax.random.fold_in(own, 1), rows)]
    offset_by = jax.random.randint(jax.random.fold_in(own, 2), (rows, 1), 0, top)
    return jnp.take_along_axis(listing, (jnp.arange(top)[None, :] + offset_by) % top, axis=1)


def load_shares(count, total, reach, lean, full):
    loads = [(1 << 20) // math.isqrt(grade ** lean) + 1 for grade in range(1, count + 1)]
    largest = reach if full else min(reach, max(-(-total // count), total * loads[0] // sum(loads)))
    least = 1 if total - largest >= count - 1 else 0
    holding, spare = [largest] + [least] * (count - 1), total - largest - least * (count - 1)
    while spare > 0:
        free = [i for i in range(1, count) if holding[i] < largest] or [i for i in range(1, count) if holding[i] < reach]
        pool, remaining = sum([loads[i] for i in free]), spare
        for i in free:
            more = min(reach - holding[i], max(1, remaining * loads[i] // pool), spare)
            holding[i] = holding[i] + more
            spare = spare - more
    return np.array(holding)


def noise(key, shape, deviation, most, cuts=(), held_as=jnp.bfloat16):
    result = jax.random.normal(key, shape, jnp.float32) * deviation
    if len(cuts) > 0:
        result = shard_levels(key, shape, cuts, -0.22, 0.18) * result
    return jnp.clip(result, min=-most, max=most).astype(held_as)


def noise_with(rng, extent, width, bound, cuts, heavy, held_as=jnp.bfloat16):
    values = width * jax.random.normal(rng, extent, jnp.float32)
    if cuts:
        values = values * shard_levels(rng, extent, cuts, -0.22, 0.18)
    return jnp.clip(raised(values, jax.random.fold_in(rng, 3), *heavy), -bound, bound).astype(held_as)


def setup_inputs(seed: int = 0) -> dict:
    seeds = jax.random.split(jax.random.key(seed), 7)
    ainv_anc = noise(seeds[0], (ORDER, ORDER), 1.0, 6.0, ((0, 8), (1, 16)))
    l_panel = noise_with(seeds[1], (PANEL, ORDER), (ORDER // 2) ** -0.5, 0.078125, ((0, 16), (1, 8)), (1, 0, 16, 2.0))
    diag_inv = noise(seeds[2], (PANEL, W), 1.0, 6.0, ((0, 16), (1, 8)), jnp.float32)
    struct_mask = touch_ends((jax.random.randint(seeds[3], (NS, NBLK), 0, 2) < 1).astype(jnp.int32), jax.random.fold_in(seeds[3], 1), 0, 1)
    pieces = noise(seeds[4], (PIECES, TR, TC), 1.0, 6.0, ((0, 128),), jnp.float32)
    tile_owner_keys = jax.random.split(jax.random.fold_in(seeds[5], 1), PIECES // TPD)
    tile_owner_turns = jax.random.permutation(jax.random.fold_in(seeds[5], 3), PIECES // TPD)
    tile_owner = jax.vmap(lambda own, number: shared_out(jax.random.fold_in(seeds[5], 2), own, number, TPD, DEVICES, 1, SLOT, 2))(tile_owner_keys, tile_owner_turns).reshape((PIECES, 1))
    return dict(ainv_anc=ainv_anc, l_panel=l_panel, diag_inv=diag_inv, struct_mask=struct_mask, pieces=pieces, tile_owner=tile_owner)


def mask_panel(l_panel, struct_mask):
    blocks = jnp.repeat(struct_mask, AB, axis=1)
    keep = blocks[:, None, :] > 0
    shaped = l_panel.reshape(NS, W, ORDER)
    masked = jnp.where(keep, shaped, jnp.zeros_like(shaped))
    return masked.reshape(NS * W, ORDER), keep


def reference(ainv_anc, l_panel, diag_inv, struct_mask, pieces, tile_owner):
    masked_panel, keep = mask_panel(l_panel, struct_mask)
    group_width = ORDER // N_COL

    def add_group(index, total):
        begin = (index * group_width).astype(jnp.int32)
        panel_cols = lax.dynamic_slice_in_dim(masked_panel, begin, group_width, 1)
        inverse_cols = lax.dynamic_slice_in_dim(ainv_anc, begin, group_width, 1)
        term = lax.dot_general(panel_cols, inverse_cols, (((1,), (1,)), ((), ())), preferred_element_type=jnp.float32)
        rounded = lax.optimization_barrier(term.astype(jnp.bfloat16))
        return total + rounded.astype(jnp.float32)

    product = lax.fori_loop(0, N_COL, add_group, jnp.zeros((NS * W, ORDER), jnp.float32))
    shaped = product.reshape(NS, W, ORDER)
    upper_rows = jnp.where(keep, -shaped, jnp.zeros_like(shaped)).reshape(NS * W, ORDER).astype(jnp.bfloat16)
    diag_blocks = []
    for supernode in range(NS):
        upper_part = upper_rows[supernode * W:(supernode + 1) * W]
        panel_part = masked_panel[supernode * W:(supernode + 1) * W]
        diag_blocks.append(lax.dot_general(upper_part, panel_part, (((1,), (1,)), ((), ())), preferred_element_type=jnp.float32))
    ainv_diag = diag_inv - jnp.concatenate(diag_blocks, axis=0)
    devices_all = N_ROW * N_COL
    owners = tile_owner[:, 0].reshape(devices_all, TPD)
    onehot = (owners[:, :, None] == jnp.arange(devices_all, dtype=jnp.int32)[None, None, :]).astype(jnp.int32)
    earlier = jnp.cumsum(onehot, axis=1) - onehot
    rank_in_dest = jnp.sum(earlier * onehot, axis=2)
    source = jnp.arange(devices_all, dtype=jnp.int32)[:, None]
    slot_index = ((owners * devices_all + source) * SLOT + rank_in_dest).reshape(-1).astype(jnp.int32)
    moved = jnp.zeros((devices_all * devices_all * SLOT, TR, TC), jnp.float32).at[slot_index].set(pieces)
    return upper_rows, ainv_diag, moved
```

```python
import jax
import jax.numpy as jnp
from jax import lax
from jax.experimental import pallas as pl
from jax.experimental.pallas import tpu as pltpu
from jax.sharding import PartitionSpec as P

W = 768
AB = 128
SLOT = 3
SIDE = 4
PB = 96
HALF = 1536
QUART = 768
TILE = 256
BF16, F32 = jnp.bfloat16, jnp.float32


def pack_kernel(owner_ref, pieces_ref, out_ref, count_ref):
    devices = out_ref.shape[0] // SLOT

    def clear(i, _):
        out_ref[pl.ds(i * 8, 8)] = jnp.zeros((8, *out_ref.shape[1:]), out_ref.dtype)
        return 0

    lax.fori_loop(0, out_ref.shape[0] // 8, clear, 0)

    def reset(i, _):
        count_ref[i] = 0
        return 0

    lax.fori_loop(0, devices, reset, 0)

    def place(p, _):
        owner = owner_ref[p]
        rank = count_ref[owner]
        count_ref[owner] = rank + 1
        out_ref[owner * SLOT + rank] = pieces_ref[p].astype(out_ref.dtype)
        return 0

    lax.fori_loop(0, pieces_ref.shape[0], place, 0)


def packed(owners, pieces, devices):
    shape = (devices * SLOT, *pieces.shape[1:])
    return pl.pallas_call(
        pack_kernel,
        out_shape=jax.ShapeDtypeStruct(shape, BF16),
        in_specs=[
            pl.BlockSpec(memory_space=pltpu.SMEM),
            pl.BlockSpec(memory_space=pltpu.VMEM),
        ],
        out_specs=pl.BlockSpec(memory_space=pltpu.VMEM),
        scratch_shapes=[pltpu.SMEM((devices,), jnp.int32)],
        name="pack",
    )(owners, pieces)


def invert_kernel(
    mask_ref, a_hbm, panel_ref, dinv_ref, upper_ref, diag_ref,
    zbuf, lm, a, part, in1, tot, in2, usend, ubuf, sendd, recvd,
    a_sem, z_ssem, z_rsem, l_ssem, l_rsem, f_ssem, f_rsem,
    p1_ssem, p1_rsem, p2_ssem, p2_rsem, u_ssem, u_rsem, d_ssem, d_rsem,
):
    r, c = lax.axis_index("row"), lax.axis_index("col")
    z, k = r // 2, r % 2
    y, x = c // SIDE, c % SIDE
    node = c // (W // PB)
    started = []

    def at(row, col):
        return {"row": row, "col": col}

    def send(src, dst, ssem, rsem, row, col):
        return pltpu.make_async_remote_copy(
            src_ref=src, dst_ref=dst, send_sem=ssem, recv_sem=rsem,
            device_id=at(row, col), device_id_type=pl.DeviceIdType.MESH,
        )

    def go(*args):
        copy = send(*args)
        copy.start()
        started.append(copy)

    def arrived(dst, sem):
        send(dst, dst, sem, sem, r, c).wait_recv()

    a_copy = pltpu.make_async_copy(a_hbm, a, a_sem)
    a_copy.start()

    blocks = panel_ref.shape[1] // AB
    for b in range(blocks):
        keep = jnp.full((PB, AB), mask_ref[node, r * blocks + b], jnp.int32) > 0
        value = panel_ref[:, b * AB : (b + 1) * AB].astype(F32)
        h, o = divmod(b * AB, HALF)
        zbuf[z, h, :, o : o + AB] = jnp.where(keep, value, 0.0).astype(BF16)

    zp, zm, zo = (z + 1) % SIDE, (z + 3) % SIDE, (z + 2) % SIDE
    up, down = 2 * zp + k, 2 * zm + k
    go(zbuf.at[z, 0], zbuf.at[z, 0], z_ssem.at[0], z_rsem.at[0], up, c)
    go(zbuf.at[z, 1], zbuf.at[z, 1], z_ssem.at[1], z_rsem.at[1], down, c)
    go(zbuf.at[z, 1], zbuf.at[z, 1], z_ssem.at[2], z_rsem.at[2], up, c)
    go(zbuf.at[z, 0], zbuf.at[z, 0], z_ssem.at[3], z_rsem.at[3], down, c)

    core = (x + y) % 2

    def own_block(zs, h):
        return (SIDE * zs + 2 * k + h == c) & (k == core)

    spread = []

    def to_column(n, zs, h):
        copy = send(
            zbuf.at[zs, h], lm.at[c], l_ssem.at[n], l_rsem.at[c],
            2 * z + core, SIDE * zs + 2 * k + h,
        )
        mine = own_block(zs, h)

        @pl.when(mine)
        def _():
            lm[c] = zbuf[zs, h]

        @pl.when(jnp.logical_not(mine))
        def _():
            copy.start()

        spread.append((copy, mine))

    to_column(0, z, 0)
    to_column(1, z, 1)
    arrived(zbuf.at[zm, 0], z_rsem.at[0])
    go(zbuf.at[zm, 0], zbuf.at[zm, 0], z_ssem.at[4], z_rsem.at[4], up, c)
    arrived(zbuf.at[zp, 1], z_rsem.at[1])
    go(zbuf.at[zp, 1], zbuf.at[zp, 1], z_ssem.at[5], z_rsem.at[5], down, c)
    to_column(2, zm, 0)
    to_column(3, zp, 1)
    arrived(zbuf.at[zm, 1], z_rsem.at[2])
    to_column(4, zm, 1)
    arrived(zbuf.at[zp, 0], z_rsem.at[3])
    to_column(5, zp, 0)
    arrived(zbuf.at[zo, 0], z_rsem.at[4])
    to_column(6, zo, 0)
    arrived(zbuf.at[zo, 1], z_rsem.at[5])
    to_column(7, zo, 1)

    other = 2 * z + 1 - k

    def nth(n, parity):
        yy, xx = n // 2, n % 2
        return SIDE * yy + 2 * xx + (yy + parity) % 2

    def hand_on(n, _):
        b = nth(n, k)

        @pl.when(jnp.logical_not((b == c) & (x // 2 == k)))
        def _():
            arrived(lm.at[b], l_rsem.at[b])

        send(lm.at[b], lm.at[b], f_ssem.at[n], f_rsem.at[b], other, c).start()
        return 0

    lax.fori_loop(0, 8, hand_on, 0)

    def take(n, _):
        b = nth(n, 1 - k)
        arrived(lm.at[b], f_rsem.at[b])
        return 0

    lax.fori_loop(0, 8, take, 0)
    a_copy.wait()

    place = (x, y)

    def neighbour(axis, step):
        if axis == 0:
            return r, SIDE * y + (x + step) % SIDE
        return r, SIDE * ((y + step) % SIDE) + x

    FAR, NEXT, LAST, OWN = range(4)

    def multiply(half, slot, dest):
        across, along = (SIDE, 1) if half == 0 else (1, SIDE)

        def tile(t, _):
            rows = jnp.concatenate([lm[j * across + dest * along] for j in range(SIDE)], axis=0)
            cols = a[pl.ds(pl.multiple_of(half * HALF + t * TILE, TILE), TILE), :]
            value = lax.dot_general(rows, cols, (((1,), (1,)), ((), ())), preferred_element_type=F32)
            per = QUART // TILE
            part[half, slot, t // per, :, pl.ds(pl.multiple_of((t % per) * TILE, TILE), TILE)] = value.astype(BF16)
            return 0

        lax.fori_loop(0, HALF // TILE, tile, 0)

    def hop1(half, slot, piece, n, step):
        go(
            part.at[half, slot, piece], in1.at[half, n], p1_ssem.at[half, n], p1_rsem.at[half, n],
            *neighbour(half, step),
        )

    def add1(half, slot, piece, n):
        arrived(in1.at[half, n], p1_rsem.at[half, n])

        def rows(i, _):
            s = pl.ds(pl.multiple_of(i * 32, 32), 32)
            value = part[half, slot, piece, s, :].astype(F32) + in1[half, n, s, :].astype(F32)
            part[half, slot, piece, s, :] = value.astype(BF16)
            return 0

        lax.fori_loop(0, SIDE * PB // 32, rows, 0)

    for half in range(2):
        multiply(half, FAR, (place[half] + 2) % SIDE)
        hop1(half, FAR, 0, 0, 1)
        hop1(half, FAR, 1, 1, 3)
    for half in range(2):
        multiply(half, NEXT, (place[half] + 1) % SIDE)
        hop1(half, NEXT, 1, 3, 1)
        multiply(half, LAST, (place[half] + 3) % SIDE)
        hop1(half, LAST, 0, 5, 3)
    for half in range(2):
        add1(half, NEXT, 0, 0)
        hop1(half, NEXT, 0, 2, 1)
        add1(half, LAST, 1, 1)
        hop1(half, LAST, 1, 4, 3)
    for half in range(2):
        multiply(half, OWN, place[half])

    def hop2(half, group, piece, n, step):
        go(
            tot.at[half, group, piece], in2.at[half, n], p2_ssem.at[half, n], p2_rsem.at[half, n],
            *neighbour(1 - half, step),
        )

    def add2(half, group, piece, n):
        arrived(in2.at[half, n], p2_rsem.at[half, n])
        value = tot[half, group, piece].astype(F32) + in2[half, n].astype(F32)
        tot[half, group, piece] = value.astype(BF16)

    for half in range(2):
        q = place[1 - half]
        for n in (3, 5, 2, 4):
            arrived(in1.at[half, n], p1_rsem.at[half, n])

        def sums(i, _, half=half):
            s = pl.ds(pl.multiple_of(i * PB, PB), PB)
            for piece, (m, n) in enumerate(((2, 5), (3, 4))):
                value = part[half, OWN, piece, s, :].astype(F32) + in1[half, m, s, :].astype(F32)
                tot[half, i, piece] = (value + in1[half, n, s, :].astype(F32)).astype(BF16)
            return 0

        lax.fori_loop(0, SIDE, sums, 0)
        hop2(half, (q + 2) % SIDE, 0, 0, 1)
        hop2(half, (q + 2) % SIDE, 1, 1, 3)
        hop2(half, (q + 1) % SIDE, 1, 3, 1)
        hop2(half, (q + 3) % SIDE, 0, 5, 3)
    for half in range(2):
        q = place[1 - half]
        add2(half, (q + 1) % SIDE, 0, 0)
        hop2(half, (q + 1) % SIDE, 0, 2, 1)
        add2(half, (q + 3) % SIDE, 1, 1)
        hop2(half, (q + 3) % SIDE, 1, 4, 3)

    row_to, e = c // 2, c % 2
    handed = []
    for half in range(2):
        q = place[1 - half]
        for n in (3, 5, 2, 4):
            arrived(in2.at[half, n], p2_rsem.at[half, n])
        for piece, (m, n) in enumerate(((2, 5), (3, 4))):
            for b in range(QUART // AB):
                s = slice(b * AB, (b + 1) * AB)
                o = piece * QUART + b * AB
                keep = mask_ref[node, r * blocks + (half * HALF + o) // AB]
                value = tot[half, q, piece, :, s].astype(F32) + in2[half, m, :, s].astype(F32)
                value = value + in2[half, n, :, s].astype(F32)
                value = jnp.where(jnp.full((PB, AB), keep, jnp.int32) > 0, -value, 0.0).astype(BF16)
                upper_ref[:, half * HALF + o : half * HALF + o + AB] = value
                usend[half, :, o : o + AB] = value
        copy = send(
            usend.at[half], ubuf.at[e], u_ssem.at[half], u_rsem.at[e], row_to, 2 * r + half
        )
        mine = (row_to == r) & (e == half)

        @pl.when(mine)
        def _(half=half):
            ubuf[e] = usend[half]

        @pl.when(jnp.logical_not(mine))
        def _(copy=copy):
            copy.start()

        handed.append((copy, mine))

    for s in range(2):

        @pl.when(jnp.logical_not((row_to == r) & (e == s)))
        def _(s=s):
            arrived(ubuf.at[s], u_rsem.at[s])

    mine_k = r // 4

    def owner_part(i, _):
        rows = jnp.concatenate([ubuf[0], ubuf[1]], axis=0)
        value = lax.dot_general(
            rows, lm[mine_k * (W // PB) + i], (((1,), (1,)), ((), ())), preferred_element_type=F32
        )
        value = jnp.concatenate([value, jnp.zeros((2 * PB, AB - PB), F32)], axis=1).astype(BF16)
        for s in range(2):
            sendd[i, s] = value[s * PB : (s + 1) * PB]
            mine = (i == r) & (2 * r + s == c)

            @pl.when(mine)
            def _(s=s):
                recvd[c] = sendd[i, s]

            @pl.when(jnp.logical_not(mine))
            def _(s=s):
                send(
                    sendd.at[i, s], recvd.at[c], d_ssem.at[i, s], d_rsem.at[c], i, 2 * r + s
                ).start()

        return 0

    lax.fori_loop(0, W // PB, owner_part, 0)

    diag_ref[...] = dinv_ref[...]

    def collect(i, _):
        @pl.when(jnp.logical_not((row_to == r) & (i == c)))
        def _():
            arrived(recvd.at[i], d_rsem.at[i])

        diag_ref[...] = diag_ref[...] - recvd[i, :, :PB].astype(F32)
        return 0

    lax.fori_loop(0, SIDE * SIDE, collect, 0)

    for copy in started:
        copy.wait_send()
    for copy, mine in spread + handed:

        @pl.when(jnp.logical_not(mine))
        def _(copy=copy):
            copy.wait_send()

    def drain(n, _):
        b = nth(n, k)
        send(lm.at[b], lm.at[b], f_ssem.at[n], f_rsem.at[b], other, c).wait_send()
        for s in range(2):

            @pl.when(jnp.logical_not((n == r) & (2 * r + s == c)))
            def _(s=s):
                send(
                    sendd.at[n, s], recvd.at[c], d_ssem.at[n, s], d_rsem.at[c], n, 2 * r + s
                ).wait_send()

        return 0

    lax.fori_loop(0, 8, drain, 0)


def inverted(struct_mask, ainv_anc, l_panel, diag_inv):
    rows, width = l_panel.shape
    vmem, dma = pltpu.VMEM, pltpu.SemaphoreType.DMA
    spec = pl.BlockSpec(memory_space=pltpu.VMEM)
    return pl.pallas_call(
        invert_kernel,
        out_shape=(
            jax.ShapeDtypeStruct((rows, width), BF16),
            jax.ShapeDtypeStruct(diag_inv.shape, F32),
        ),
        in_specs=[
            pl.BlockSpec(memory_space=pltpu.SMEM),
            pl.BlockSpec(memory_space=pl.ANY),
            spec,
            spec,
        ],
        out_specs=(spec, spec),
        scratch_shapes=[
            vmem((SIDE, 2, PB, HALF), BF16),
            vmem((SIDE * SIDE, PB, HALF), BF16),
            vmem(ainv_anc.shape, BF16),
            vmem((2, 4, 2, SIDE * PB, QUART), BF16),
            vmem((2, 6, SIDE * PB, QUART), BF16),
            vmem((2, SIDE, 2, PB, QUART), BF16),
            vmem((2, 6, PB, QUART), BF16),
            vmem((2, PB, HALF), BF16),
            vmem((2, PB, HALF), BF16),
            vmem((8, 2, PB, AB), BF16),
            vmem((SIDE * SIDE, PB, AB), BF16),
            dma(()),
            dma((6,)), dma((6,)),
            dma((8,)), dma((16,)),
            dma((8,)), dma((16,)),
            dma((2, 6)), dma((2, 6)),
            dma((2, 6)), dma((2, 6)),
            dma((2,)), dma((2,)),
            dma((8, 2)), dma((16,)),
        ],
        compiler_params=pltpu.CompilerParams(
            has_side_effects=True, vmem_limit_bytes=52 * 1024 * 1024
        ),
        cost_estimate=pl.CostEstimate(
            flops=100_000_000_000, bytes_accessed=12_000_000, transcendentals=0
        ),
        name="invert",
    )(struct_mask, ainv_anc, l_panel, diag_inv)


def local(ainv_anc, l_panel, diag_inv, struct_mask, pieces, tile_owner):
    devices = lax.axis_size("row") * lax.axis_size("col")
    slots = packed(tile_owner[:, 0], pieces, devices)
    parts = slots.reshape(devices, SLOT, *pieces.shape[1:])
    arrived = lax.all_to_all(parts, ("row", "col"), split_axis=0, concat_axis=0, tiled=True)
    upper, diag = inverted(struct_mask, ainv_anc, l_panel, diag_inv)
    moved = arrived.astype(F32).reshape(slots.shape)
    return upper, diag, moved


def solution(mesh):
    in_specs = (
        P("row", "col"),
        P("col", "row"),
        P("col", "row"),
        P(),
        P(("row", "col"), None, None),
        P(("row", "col"), None),
    )
    out_specs = (P("col", "row"), P("col", "row"), P(("row", "col"), None, None))
    return jax.shard_map(local, mesh=mesh, in_specs=in_specs, out_specs=out_specs, check_vma=False)
```

```python
import jax
import jax.numpy as jnp
from jax import lax
from jax.experimental import pallas as pl
from jax.experimental.pallas import tpu as pltpu
from jax.sharding import PartitionSpec as P

W = 768
AB = 128
SLOT = 3
SIDE = 4
PB = 96
SUBS, SUB = 6, 16
AHEAD = 2
HALF = 1536
QUART = 768
TILE = 256
BF16, F32 = jnp.bfloat16, jnp.float32


def pack_kernel(owner_ref, pieces_ref, out_ref, count_ref):
    devices = out_ref.shape[0] // SLOT

    def clear(i, _):
        out_ref[pl.ds(i * 8, 8)] = jnp.zeros((8, *out_ref.shape[1:]), out_ref.dtype)
        return 0

    lax.fori_loop(0, out_ref.shape[0] // 8, clear, 0)

    def reset(i, _):
        count_ref[i] = 0
        return 0

    lax.fori_loop(0, devices, reset, 0)

    def place(p, _):
        owner = owner_ref[p]
        rank = count_ref[owner]
        count_ref[owner] = rank + 1
        out_ref[owner * SLOT + rank] = pieces_ref[p].astype(out_ref.dtype)
        return 0

    lax.fori_loop(0, pieces_ref.shape[0], place, 0)


def packed(owners, pieces, devices):
    shape = (devices * SLOT, *pieces.shape[1:])
    return pl.pallas_call(
        pack_kernel,
        out_shape=jax.ShapeDtypeStruct(shape, BF16),
        in_specs=[
            pl.BlockSpec(memory_space=pltpu.SMEM),
            pl.BlockSpec(memory_space=pltpu.VMEM),
        ],
        out_specs=pl.BlockSpec(memory_space=pltpu.VMEM),
        scratch_shapes=[pltpu.SMEM((devices,), jnp.int32)],
        name="pack",
    )(owners, pieces)


def invert_kernel(
    mask_ref, a_hbm, panel_ref, dinv_ref, upper_ref, diag_ref,
    lmx, lm, a, part, in1, tot, in2, usend, ubuf, sendd, recvd,
    a_sem, x_ssem, x_rsem, g_ssem, l_rsem, c_ssem, f_ssem, f_rsem,
    p1_ssem, p1_rsem, p2_ssem, p2_rsem, u_ssem, u_rsem, d_ssem, d_rsem,
):
    r, c = lax.axis_index("row"), lax.axis_index("col")
    z, k = r // 2, r % 2
    y, x = c // SIDE, c % SIDE
    twin = y + 1 - 2 * (y % 2)
    node = c // (W // PB)
    started = []

    def at(row, col):
        return {"row": row, "col": col}

    def send(src, dst, ssem, rsem, row, col):
        return pltpu.make_async_remote_copy(
            src_ref=src, dst_ref=dst, send_sem=ssem, recv_sem=rsem,
            device_id=at(row, col), device_id_type=pl.DeviceIdType.MESH,
        )

    def go(*args):
        copy = send(*args)
        copy.start()
        started.append(copy)

    def arrived(dst, sem):
        send(dst, dst, sem, sem, r, c).wait_recv()

    a_copy = pltpu.make_async_copy(a_hbm, a, a_sem)
    a_copy.start()

    barrier = pltpu.get_barrier_semaphore()

    def greet(row, col):
        pl.semaphore_signal(
            barrier, inc=1, device_id=at(row, col), device_id_type=pl.DeviceIdType.MESH
        )

    def greet_plane(n, _):
        d = n // 2
        greet(2 * z + (k + n) % 2, SIDE * ((y + d // SIDE) % SIDE) + (x + d) % SIDE)
        return 0

    def greet_z(n, _):
        row = (2 * z + 2 + n) % (2 * SIDE)
        greet(row, c)
        greet(row, SIDE * twin + x)
        return 0

    lax.fori_loop(1, 2 * SIDE * SIDE, greet_plane, 0)
    lax.fori_loop(0, 2 * SIDE - 2, greet_z, 0)

    blocks = panel_ref.shape[1] // AB
    for b in range(blocks):
        keep = jnp.full((PB, AB), mask_ref[node, r * blocks + b], jnp.int32) > 0
        value = panel_ref[:, b * AB : (b + 1) * AB].astype(F32)
        h, o = divmod(b * AB, HALF)
        value = jnp.where(keep, value, 0.0).astype(BF16)
        lmx[x, h, :, :, o : o + AB] = value.reshape(SUBS, SUB, AB)

    pl.semaphore_wait(barrier, 2 * SIDE * SIDE - 1 + 2 * (2 * SIDE - 2))

    core = (x + y) % 2
    root_row = 2 * z + core

    def own_block(h):
        return (SIDE * z + 2 * k + h == c) & (k == core)

    def gather(s, wait):
        for h in range(2):
            copy = send(
                lmx.at[x, h, s], lm.at[c, s], g_ssem.at[h, s], l_rsem.at[c, s],
                root_row, SIDE * z + 2 * k + h,
            )
            mine = own_block(h)

            @pl.when(jnp.logical_not(mine))
            def _(copy=copy):
                copy.wait_send() if wait else copy.start()

            if not wait:

                @pl.when(mine)
                def _(h=h):
                    lm[c, s] = lmx[x, h, s]

    for s in range(AHEAD):
        gather(s, False)

    xp, xm, xo = (x + 1) % SIDE, (x + 3) % SIDE, (x + 2) % SIDE
    right, left = SIDE * y + xp, SIDE * y + xm
    go(lmx.at[x, 0], lmx.at[x, 0], x_ssem.at[0], x_rsem.at[0], r, right)
    go(lmx.at[x, 1], lmx.at[x, 1], x_ssem.at[1], x_rsem.at[1], r, left)
    go(lmx.at[x, 1], lmx.at[x, 1], x_ssem.at[2], x_rsem.at[2], r, right)
    go(lmx.at[x, 0], lmx.at[x, 0], x_ssem.at[3], x_rsem.at[3], r, left)

    other = 2 * z + 1 - k
    following = 2 * ((z + 1 + 2 * k) % SIDE) + k
    first, last = z == y, following // 2 == y

    def nth(n, parity):
        yy, xx = n // 2, n % 2
        return SIDE * yy + 2 * xx + (yy + parity) % 2

    def hand_on(i, _):
        n, s = i % 8, i // 8
        b = nth(n, k)

        @pl.when(jnp.logical_not(first & (b == c) & (x // 2 == k)))
        def _():
            arrived(lm.at[b, s], l_rsem.at[b, s])

        @pl.when(jnp.logical_not(last))
        def _():
            send(lm.at[b, s], lm.at[b, s], c_ssem.at[n, s], l_rsem.at[b, s], following, c).start()

        send(lm.at[b, s], lm.at[b, s], f_ssem.at[n, s], f_rsem.at[b, s], other, c).start()
        return 0

    def part_on(s, _):
        gather(s, True)

        @pl.when(s + AHEAD < SUBS)
        def _():
            gather(s + AHEAD, False)

        return lax.fori_loop(8 * s, 8 * s + 8, hand_on, 0)

    lax.fori_loop(0, SUBS // 2, part_on, 0)
    arrived(lmx.at[xm, 0], x_rsem.at[0])
    go(lmx.at[xm, 0], lmx.at[xm, 0], x_ssem.at[4], x_rsem.at[4], r, right)
    arrived(lmx.at[xp, 1], x_rsem.at[1])
    go(lmx.at[xp, 1], lmx.at[xp, 1], x_ssem.at[5], x_rsem.at[5], r, left)
    lax.fori_loop(SUBS // 2, SUBS, part_on, 0)

    def take(i, _):
        s = i // 8
        b = nth(i % 8, 1 - k)
        arrived(lm.at[b, s], f_rsem.at[b, s])
        return 0

    lax.fori_loop(0, 8 * SUBS, take, 0)
    a_copy.wait()

    place = (x, y)

    def neighbour(axis, step):
        if axis == 0:
            return r, SIDE * y + (x + step) % SIDE
        return r, SIDE * ((y + step) % SIDE) + x

    FAR, NEXT, LAST, OWN = range(4)

    def multiply(half, slot, dest):
        across, along = (SIDE, 1) if half == 0 else (1, SIDE)

        def tile(t, _):
            rows = jnp.concatenate(
                [lm[j * across + dest * along].reshape(PB, HALF) for j in range(SIDE)], axis=0
            )
            cols = a[pl.ds(pl.multiple_of(half * HALF + t * TILE, TILE), TILE), :]
            value = lax.dot_general(rows, cols, (((1,), (1,)), ((), ())), preferred_element_type=F32)
            per = QUART // TILE
            part[half, slot, t // per, :, pl.ds(pl.multiple_of((t % per) * TILE, TILE), TILE)] = value.astype(BF16)
            return 0

        lax.fori_loop(0, HALF // TILE, tile, 0)

    def hop1(half, slot, piece, n, step):
        go(
            part.at[half, slot, piece], in1.at[half, n], p1_ssem.at[half, n], p1_rsem.at[half, n],
            *neighbour(half, step),
        )

    def add1(half, slot, piece, n):
        arrived(in1.at[half, n], p1_rsem.at[half, n])

        def rows(i, _):
            s = pl.ds(pl.multiple_of(i * 32, 32), 32)
            value = part[half, slot, piece, s, :].astype(F32) + in1[half, n, s, :].astype(F32)
            part[half, slot, piece, s, :] = value.astype(BF16)
            return 0

        lax.fori_loop(0, SIDE * PB // 32, rows, 0)

    for half in range(2):
        multiply(half, FAR, (place[half] + 2) % SIDE)
        hop1(half, FAR, 0, 0, 1)
        hop1(half, FAR, 1, 1, 3)
    for half in range(2):
        multiply(half, NEXT, (place[half] + 1) % SIDE)
        hop1(half, NEXT, 1, 3, 1)
        multiply(half, LAST, (place[half] + 3) % SIDE)
        hop1(half, LAST, 0, 5, 3)
    for half in range(2):
        add1(half, NEXT, 0, 0)
        hop1(half, NEXT, 0, 2, 1)
        add1(half, LAST, 1, 1)
        hop1(half, LAST, 1, 4, 3)
    for half in range(2):
        multiply(half, OWN, place[half])

    def hop2(half, group, piece, n, step):
        go(
            tot.at[half, group, piece], in2.at[half, n], p2_ssem.at[half, n], p2_rsem.at[half, n],
            *neighbour(1 - half, step),
        )

    def add2(half, group, piece, n):
        arrived(in2.at[half, n], p2_rsem.at[half, n])
        value = tot[half, group, piece].astype(F32) + in2[half, n].astype(F32)
        tot[half, group, piece] = value.astype(BF16)

    for half in range(2):
        q = place[1 - half]
        for n in (3, 5, 2, 4):
            arrived(in1.at[half, n], p1_rsem.at[half, n])

        def sums(i, _, half=half):
            s = pl.ds(pl.multiple_of(i * PB, PB), PB)
            for piece, (m, n) in enumerate(((2, 5), (3, 4))):
                value = part[half, OWN, piece, s, :].astype(F32) + in1[half, m, s, :].astype(F32)
                tot[half, i, piece] = (value + in1[half, n, s, :].astype(F32)).astype(BF16)
            return 0

        lax.fori_loop(0, SIDE, sums, 0)
        hop2(half, (q + 2) % SIDE, 0, 0, 1)
        hop2(half, (q + 2) % SIDE, 1, 1, 3)
        hop2(half, (q + 1) % SIDE, 1, 3, 1)
        hop2(half, (q + 3) % SIDE, 0, 5, 3)
    for half in range(2):
        q = place[1 - half]
        add2(half, (q + 1) % SIDE, 0, 0)
        hop2(half, (q + 1) % SIDE, 0, 2, 1)
        add2(half, (q + 3) % SIDE, 1, 1)
        hop2(half, (q + 3) % SIDE, 1, 4, 3)

    for half in range(2):
        q = place[1 - half]
        for n in (3, 5, 2, 4):
            arrived(in2.at[half, n], p2_rsem.at[half, n])
        for piece, (m, n) in enumerate(((2, 5), (3, 4))):
            for b in range(QUART // AB):
                s = slice(b * AB, (b + 1) * AB)
                o = piece * QUART + b * AB
                keep = mask_ref[node, r * blocks + (half * HALF + o) // AB]
                value = tot[half, q, piece, :, s].astype(F32) + in2[half, m, :, s].astype(F32)
                value = value + in2[half, n, :, s].astype(F32)
                value = jnp.where(jnp.full((PB, AB), keep, jnp.int32) > 0, -value, 0.0).astype(BF16)
                upper_ref[:, half * HALF + o : half * HALF + o + AB] = value
                usend[half, :, o : o + AB] = value
        go(usend.at[half], ubuf.at[half], u_ssem.at[half], u_rsem.at[half], r, SIDE * twin + x)

    for n, (b, h) in enumerate(((xm, 1), (xp, 0), (xo, 0), (xo, 1))):
        arrived(lmx.at[b, h], x_rsem.at[2 + n])

    owner0 = (y % 2) * SIDE

    def partial(s, source):
        def one(i, _):
            value = jnp.zeros((PB, PB), F32)
            for h in range(2):
                value = value + lax.dot_general(
                    source[h], lmx[i, h].reshape(PB, HALF), (((1,), (1,)), ((), ())),
                    preferred_element_type=F32,
                )
            sendd[s, i, :, :PB] = value.astype(BF16)
            copy = send(
                sendd.at[s, i], recvd.at[r], d_ssem.at[s, i], d_rsem.at[r],
                owner0 + i, SIDE * (y, twin)[s] + x,
            )
            if s:
                copy.start()
            else:

                @pl.when(owner0 + i == r)
                def _():
                    recvd[r] = sendd[s, i]

                @pl.when(owner0 + i != r)
                def _():
                    copy.start()

            return 0

        lax.fori_loop(0, SIDE, one, 0)

    sendd[...] = jnp.zeros_like(sendd)
    partial(0, usend)
    for h in range(2):
        arrived(ubuf.at[h], u_rsem.at[h])
    partial(1, ubuf)

    diag_ref[...] = dinv_ref[...]

    def collect(i, _):
        @pl.when(jnp.logical_not((i == r) & (r // SIDE == y % 2)))
        def _():
            arrived(recvd.at[i], d_rsem.at[i])

        diag_ref[...] = diag_ref[...] - recvd[i, :, :PB].astype(F32)
        return 0

    lax.fori_loop(0, 2 * SIDE, collect, 0)

    for copy in started:
        copy.wait_send()
    def drain(i, _):
        n, s = i % 8, i // 8
        b = nth(n, k)

        @pl.when(jnp.logical_not(last))
        def _():
            send(lm.at[b, s], lm.at[b, s], c_ssem.at[n, s], l_rsem.at[b, s], following, c).wait_send()

        send(lm.at[b, s], lm.at[b, s], f_ssem.at[n, s], f_rsem.at[b, s], other, c).wait_send()
        return 0

    lax.fori_loop(0, 8 * SUBS, drain, 0)

    def drain_diag(i, _):
        for s in range(2):
            copy = send(
                sendd.at[s, i], recvd.at[r], d_ssem.at[s, i], d_rsem.at[r],
                owner0 + i, SIDE * (y, twin)[s] + x,
            )
            if s:
                copy.wait_send()
            else:

                @pl.when(owner0 + i != r)
                def _(copy=copy):
                    copy.wait_send()

        return 0

    lax.fori_loop(0, SIDE, drain_diag, 0)


def inverted(struct_mask, ainv_anc, l_panel, diag_inv):
    rows, width = l_panel.shape
    vmem, dma = pltpu.VMEM, pltpu.SemaphoreType.DMA
    spec = pl.BlockSpec(memory_space=pltpu.VMEM)
    return pl.pallas_call(
        invert_kernel,
        out_shape=(
            jax.ShapeDtypeStruct((rows, width), BF16),
            jax.ShapeDtypeStruct(diag_inv.shape, F32),
        ),
        in_specs=[
            pl.BlockSpec(memory_space=pltpu.SMEM),
            pl.BlockSpec(memory_space=pl.ANY),
            spec,
            spec,
        ],
        out_specs=(spec, spec),
        scratch_shapes=[
            vmem((SIDE, 2, SUBS, SUB, HALF), BF16),
            vmem((SIDE * SIDE, SUBS, SUB, HALF), BF16),
            vmem(ainv_anc.shape, BF16),
            vmem((2, 4, 2, SIDE * PB, QUART), BF16),
            vmem((2, 6, SIDE * PB, QUART), BF16),
            vmem((2, SIDE, 2, PB, QUART), BF16),
            vmem((2, 6, PB, QUART), BF16),
            vmem((2, PB, HALF), BF16),
            vmem((2, PB, HALF), BF16),
            vmem((2, SIDE, PB, AB), BF16),
            vmem((2 * SIDE, PB, AB), BF16),
            dma(()),
            dma((6,)), dma((6,)),
            dma((2, SUBS)), dma((16, SUBS)),
            dma((8, SUBS)), dma((8, SUBS)), dma((16, SUBS)),
            dma((2, 6)), dma((2, 6)),
            dma((2, 6)), dma((2, 6)),
            dma((2,)), dma((2,)),
            dma((2, SIDE)), dma((2 * SIDE,)),
        ],
        compiler_params=pltpu.CompilerParams(
            collective_id=0, has_side_effects=True, vmem_limit_bytes=52 * 1024 * 1024
        ),
        cost_estimate=pl.CostEstimate(
            flops=100_000_000_000, bytes_accessed=12_000_000, transcendentals=0
        ),
        name="invert",
    )(struct_mask, ainv_anc, l_panel, diag_inv)


def local(ainv_anc, l_panel, diag_inv, struct_mask, pieces, tile_owner):
    devices = lax.axis_size("row") * lax.axis_size("col")
    slots = packed(tile_owner[:, 0], pieces, devices)
    parts = slots.reshape(devices, SLOT, *pieces.shape[1:])
    arrived = lax.all_to_all(parts, ("row", "col"), split_axis=0, concat_axis=0, tiled=True)
    upper, diag = inverted(struct_mask, ainv_anc, l_panel, diag_inv)
    moved = arrived.astype(F32).reshape(slots.shape)
    return upper, diag, moved


def solution(mesh):
    in_specs = (
        P("row", "col"),
        P("col", "row"),
        P("col", "row"),
        P(),
        P(("row", "col"), None, None),
        P(("row", "col"), None),
    )
    out_specs = (P("col", "row"), P("col", "row"), P(("row", "col"), None, None))
    return jax.shard_map(local, mesh=mesh, in_specs=in_specs, out_specs=out_specs, check_vma=False)
```

```python
import jax
import jax.numpy as jnp
from jax import lax
from jax.experimental import pallas as pl
from jax.experimental.pallas import tpu as pltpu
from jax.sharding import PartitionSpec as P

W = 768
AB = 128
SLOT = 3
SIDE = 4
PB = 96
SUBS, SUB = 3, 32
EVEN = ((2, 0), (2, 2), (0, 2), (0, 0), (1, 1), (1, 3), (3, 1), (3, 3))
ODD = ((2, 1), (2, 3), (1, 2), (3, 2), (1, 0), (3, 0), (0, 1), (0, 3))
HALF = 1536
QUART = 768
TILE = 256
BF16, F32 = jnp.bfloat16, jnp.float32


def pack_kernel(owner_ref, pieces_hbm, out_ref, pieces, count_ref, slot_ref, sems):
    parts = pieces.shape[0]
    per = pieces.shape[1]
    copies = [
        pltpu.make_async_copy(pieces_hbm.at[pl.ds(i * per, per)], pieces.at[i], sems.at[i])
        for i in range(parts)
    ]
    for copy in copies:
        copy.start()

    def reset(i, _):
        count_ref[i] = 0
        return 0

    lax.fori_loop(0, out_ref.shape[0] // SLOT, reset, 0, unroll=8)

    def number(p, _):
        owner = owner_ref[p]
        rank = count_ref[owner]
        count_ref[owner] = rank + 1
        slot_ref[p] = owner * SLOT + rank
        return 0

    lax.fori_loop(0, parts * per, number, 0, unroll=4)

    def clear(i, _):
        out_ref[pl.ds(i * 16, 16)] = jnp.zeros((16, *out_ref.shape[1:]), out_ref.dtype)
        return 0

    lax.fori_loop(0, out_ref.shape[0] // 16, clear, 0)

    for i in range(parts):
        copies[i].wait()

        def place(p, _, i=i):
            out_ref[slot_ref[i * per + p]] = pieces[i, p].astype(out_ref.dtype)
            return 0

        lax.fori_loop(0, per, place, 0, unroll=8)


def packed(owners, pieces, devices):
    count, *inside = pieces.shape
    parts = 4
    return pl.pallas_call(
        pack_kernel,
        out_shape=jax.ShapeDtypeStruct((devices * SLOT, *inside), BF16),
        in_specs=[
            pl.BlockSpec(memory_space=pltpu.SMEM),
            pl.BlockSpec(memory_space=pl.ANY),
        ],
        out_specs=pl.BlockSpec(memory_space=pltpu.VMEM),
        scratch_shapes=[
            pltpu.VMEM((parts, count // parts, *inside), pieces.dtype),
            pltpu.SMEM((devices,), jnp.int32),
            pltpu.SMEM((count,), jnp.int32),
            pltpu.SemaphoreType.DMA((parts,)),
        ],
        name="pack",
    )(owners, pieces)


def invert_kernel(
    mask_ref, a_hbm, panel_ref, dinv_ref, upper_ref, diag_ref,
    lmx, lm, a, part, in1, tot, in2, usend, ubuf, sendd, recvd,
    a_sem, x_ssem, x_rsem, g_ssem, l_rsem, c_ssem, f_ssem, f_rsem,
    p1_ssem, p1_rsem, p2_ssem, p2_rsem, u_ssem, u_rsem, d_ssem, d_rsem,
):
    r, c = lax.axis_index("row"), lax.axis_index("col")
    z, k = r // 2, r % 2
    y, x = c // SIDE, c % SIDE
    twin = y + 1 - 2 * (y % 2)
    node = c // (W // PB)
    started = []

    def at(row, col):
        return {"row": row, "col": col}

    def send(src, dst, ssem, rsem, row, col):
        return pltpu.make_async_remote_copy(
            src_ref=src, dst_ref=dst, send_sem=ssem, recv_sem=rsem,
            device_id=at(row, col), device_id_type=pl.DeviceIdType.MESH,
        )

    def go(*args):
        copy = send(*args)
        copy.start()
        started.append(copy)

    def arrived(dst, sem):
        send(dst, dst, sem, sem, r, c).wait_recv()

    a_copy = pltpu.make_async_copy(a_hbm, a, a_sem)
    a_copy.start()

    barrier = pltpu.get_barrier_semaphore()

    def greet(row, col):
        pl.semaphore_signal(
            barrier, inc=1, device_id=at(row, col), device_id_type=pl.DeviceIdType.MESH
        )

    def greet_plane(n, _):
        d = n // 2
        greet(2 * z + (k + n) % 2, SIDE * ((y + d // SIDE) % SIDE) + (x + d) % SIDE)
        return 0

    def greet_z(n, _):
        row = (2 * z + 2 + n) % (2 * SIDE)
        greet(row, c)
        greet(row, SIDE * twin + x)
        return 0

    lax.fori_loop(1, 2 * SIDE * SIDE, greet_plane, 0)
    lax.fori_loop(0, 2 * SIDE - 2, greet_z, 0)

    blocks = panel_ref.shape[1] // AB
    for b in range(blocks):
        keep = jnp.full((PB, AB), mask_ref[node, r * blocks + b], jnp.int32) > 0
        value = panel_ref[:, b * AB : (b + 1) * AB].astype(F32)
        h, o = divmod(b * AB, HALF)
        value = jnp.where(keep, value, 0.0).astype(BF16)
        lmx[x, h, :, :, o : o + AB] = value.reshape(SUBS, SUB, AB)

    pl.semaphore_wait(barrier, 2 * SIDE * SIDE - 1 + 2 * (2 * SIDE - 2))

    core = (x + y) % 2
    root_row = 2 * z + core

    def own_block(h):
        return (SIDE * z + 2 * k + h == c) & (k == core)

    def gather(h):
        return [
            send(
                lmx.at[x, h, s], lm.at[c, s], g_ssem.at[h, s], l_rsem.at[c, s],
                root_row, SIDE * z + 2 * k + h,
            )
            for s in range(SUBS)
        ]

    def soon(h):
        far_x = (x + SIDE - 2 * k - h) % SIDE == 2
        far_y = (y + SIDE - z) % SIDE == 2
        return far_x | far_y | (y == z)

    for h in range(2):

        @pl.when(own_block(h))
        def _(h=h):
            for s in range(SUBS):
                lm[c, s] = lmx[x, h, s]

        @pl.when(soon(h) & jnp.logical_not(own_block(h)))
        def _(h=h):
            for copy in gather(h):
                copy.start()

    xp, xm, xo = (x + 1) % SIDE, (x + 3) % SIDE, (x + 2) % SIDE
    right, left = SIDE * y + xp, SIDE * y + xm
    go(lmx.at[x, 0], lmx.at[x, 0], x_ssem.at[0], x_rsem.at[0], r, right)
    go(lmx.at[x, 1], lmx.at[x, 1], x_ssem.at[1], x_rsem.at[1], r, left)
    passed_on = (
        send(lmx.at[xm, 0], lmx.at[xm, 0], x_ssem.at[4], x_rsem.at[4], r, right),
        send(lmx.at[xp, 1], lmx.at[xp, 1], x_ssem.at[5], x_rsem.at[5], r, left),
    )
    started.extend(passed_on)

    def pass_on():
        arrived(lmx.at[xm, 0], x_rsem.at[0])
        passed_on[0].start()
        arrived(lmx.at[xp, 1], x_rsem.at[1])
        passed_on[1].start()

    @pl.when(y != z)
    def _():
        pass_on()
        for h in range(2):

            @pl.when(jnp.logical_not(soon(h)))
            def _(h=h):
                for copy in gather(h):
                    copy.start()

    other = 2 * z + 1 - k
    following = 2 * ((z + 1 + 2 * k) % SIDE) + k
    first, last = z == y, following // 2 == y

    def nth(n, mine):
        odd = (x + y + k + 1 - mine) % 2
        dx = EVEN[n][0] + odd * (ODD[n][0] - EVEN[n][0])
        dy = EVEN[n][1] + odd * (ODD[n][1] - EVEN[n][1])
        return SIDE * ((y + dy) % SIDE) + (x + dx) % SIDE

    def onward(n, s):
        b = nth(n, 1)
        return (
            send(lm.at[b, s], lm.at[b, s], c_ssem.at[n, s], l_rsem.at[b, s], following, c),
            send(lm.at[b, s], lm.at[b, s], f_ssem.at[n, s], f_rsem.at[b, s], other, c),
        )

    def hand_on(n, s):
        b = nth(n, 1)

        @pl.when(jnp.logical_not(first & (b == c) & (x // 2 == k)))
        def _():
            arrived(lm.at[b, s], l_rsem.at[b, s])

        chain, across = onward(n, s)

        @pl.when(jnp.logical_not(last))
        def _():
            chain.start()

        across.start()

    def every_part(n, act):
        def one(s, _):
            act(n, s)
            return 0

        lax.fori_loop(0, SUBS, one, 0)

    def take(n, s):
        b = nth(n, 0)
        arrived(lm.at[b, s], f_rsem.at[b, s])

    for n in range(4):
        every_part(n, hand_on)

    @pl.when(y == z)
    def _():
        pass_on()

    go(lmx.at[x, 1], lmx.at[x, 1], x_ssem.at[2], x_rsem.at[2], r, right)
    go(lmx.at[x, 0], lmx.at[x, 0], x_ssem.at[3], x_rsem.at[3], r, left)
    for n in range(4):
        every_part(n, take)
    a_copy.wait()

    place = (x, y)

    def neighbour(axis, step):
        if axis == 0:
            return r, SIDE * y + (x + step) % SIDE
        return r, SIDE * ((y + step) % SIDE) + x

    FAR, NEXT, LAST, OWN = range(4)

    def multiply(half, slot, dest, blocks_due=()):
        across, along = (SIDE, 1) if half == 0 else (1, SIDE)

        def tile(t, _):
            rows = jnp.concatenate(
                [lm[j * across + dest * along].reshape(PB, HALF) for j in range(SIDE)], axis=0
            )
            cols = a[pl.ds(pl.multiple_of(half * HALF + t * TILE, TILE), TILE), :]
            value = lax.dot_general(rows, cols, (((1,), (1,)), ((), ())), preferred_element_type=F32)
            per = QUART // TILE
            part[half, slot, t // per, :, pl.ds(pl.multiple_of((t % per) * TILE, TILE), TILE)] = value.astype(BF16)
            return 0

        if not blocks_due:
            lax.fori_loop(0, HALF // TILE, tile, 0)
        for i, n in enumerate(blocks_due):

            def tile_and_part(s, _, i=i, n=n):
                tile(SUBS * i + s, 0)
                hand_on(n, s)
                return 0

            lax.fori_loop(0, SUBS, tile_and_part, 0)

    def hop1(half, slot, piece, n, step):
        go(
            part.at[half, slot, piece], in1.at[half, n], p1_ssem.at[half, n], p1_rsem.at[half, n],
            *neighbour(half, step),
        )

    def add1(half, slot, piece, n):
        arrived(in1.at[half, n], p1_rsem.at[half, n])

        def rows(i, _):
            s = pl.ds(pl.multiple_of(i * 32, 32), 32)
            value = part[half, slot, piece, s, :].astype(F32) + in1[half, n, s, :].astype(F32)
            part[half, slot, piece, s, :] = value.astype(BF16)
            return 0

        lax.fori_loop(0, SIDE * PB // 32, rows, 0)

    for half in range(2):
        multiply(half, FAR, (place[half] + 2) % SIDE, (4 + 2 * half, 5 + 2 * half))
        hop1(half, FAR, 0, 0, 1)
        hop1(half, FAR, 1, 1, 3)
    for n in range(4, 8):
        every_part(n, take)
    for half in range(2):
        multiply(half, NEXT, (place[half] + 1) % SIDE)
        hop1(half, NEXT, 1, 3, 1)
        multiply(half, LAST, (place[half] + 3) % SIDE)
        hop1(half, LAST, 0, 5, 3)
    for half in range(2):
        add1(half, NEXT, 0, 0)
        hop1(half, NEXT, 0, 2, 1)
        add1(half, LAST, 1, 1)
        hop1(half, LAST, 1, 4, 3)
    for half in range(2):
        multiply(half, OWN, place[half])

    def hop2(half, group, piece, n, step):
        go(
            tot.at[half, group, piece], in2.at[half, n], p2_ssem.at[half, n], p2_rsem.at[half, n],
            *neighbour(1 - half, step),
        )

    def add2(half, group, piece, n):
        arrived(in2.at[half, n], p2_rsem.at[half, n])
        value = tot[half, group, piece].astype(F32) + in2[half, n].astype(F32)
        tot[half, group, piece] = value.astype(BF16)

    for half in range(2):
        q = place[1 - half]
        for n in (3, 5, 2, 4):
            arrived(in1.at[half, n], p1_rsem.at[half, n])

        def sums(i, _, half=half):
            s = pl.ds(pl.multiple_of(i * PB, PB), PB)
            for piece, (m, n) in enumerate(((2, 5), (3, 4))):
                value = part[half, OWN, piece, s, :].astype(F32) + in1[half, m, s, :].astype(F32)
                tot[half, i, piece] = (value + in1[half, n, s, :].astype(F32)).astype(BF16)
            return 0

        lax.fori_loop(0, SIDE, sums, 0)
        hop2(half, (q + 2) % SIDE, 0, 0, 1)
        hop2(half, (q + 2) % SIDE, 1, 1, 3)
        hop2(half, (q + 1) % SIDE, 1, 3, 1)
        hop2(half, (q + 3) % SIDE, 0, 5, 3)
    for half in range(2):
        q = place[1 - half]
        add2(half, (q + 1) % SIDE, 0, 0)
        hop2(half, (q + 1) % SIDE, 0, 2, 1)
        add2(half, (q + 3) % SIDE, 1, 1)
        hop2(half, (q + 3) % SIDE, 1, 4, 3)

    for half in range(2):
        q = place[1 - half]
        for n in (3, 5, 2, 4):
            arrived(in2.at[half, n], p2_rsem.at[half, n])
        for piece, (m, n) in enumerate(((2, 5), (3, 4))):
            for b in range(QUART // AB):
                s = slice(b * AB, (b + 1) * AB)
                o = piece * QUART + b * AB
                keep = mask_ref[node, r * blocks + (half * HALF + o) // AB]
                value = tot[half, q, piece, :, s].astype(F32) + in2[half, m, :, s].astype(F32)
                value = value + in2[half, n, :, s].astype(F32)
                value = jnp.where(jnp.full((PB, AB), keep, jnp.int32) > 0, -value, 0.0).astype(BF16)
                upper_ref[:, half * HALF + o : half * HALF + o + AB] = value
                usend[half, :, o : o + AB] = value
        go(usend.at[half], ubuf.at[half], u_ssem.at[half], u_rsem.at[half], r, SIDE * twin + x)

    for n, (b, h) in enumerate(((xm, 1), (xp, 0), (xo, 0), (xo, 1))):
        arrived(lmx.at[b, h], x_rsem.at[2 + n])

    owner0 = (y % 2) * SIDE

    def partial(s, source):
        def one(i, _):
            value = jnp.zeros((PB, PB), F32)
            for h in range(2):
                value = value + lax.dot_general(
                    source[h], lmx[i, h].reshape(PB, HALF), (((1,), (1,)), ((), ())),
                    preferred_element_type=F32,
                )
            sendd[s, i, :, :PB] = value.astype(BF16)
            copy = send(
                sendd.at[s, i], recvd.at[r], d_ssem.at[s, i], d_rsem.at[r],
                owner0 + i, SIDE * (y, twin)[s] + x,
            )
            if s:
                copy.start()
            else:

                @pl.when(owner0 + i == r)
                def _():
                    recvd[r] = sendd[s, i]

                @pl.when(owner0 + i != r)
                def _():
                    copy.start()

            return 0

        lax.fori_loop(0, SIDE, one, 0)

    sendd[...] = jnp.zeros_like(sendd)
    partial(0, usend)
    for h in range(2):
        arrived(ubuf.at[h], u_rsem.at[h])
    partial(1, ubuf)

    diag_ref[...] = dinv_ref[...]

    def collect(i, _):
        @pl.when(jnp.logical_not((i == r) & (r // SIDE == y % 2)))
        def _():
            arrived(recvd.at[i], d_rsem.at[i])

        diag_ref[...] = diag_ref[...] - recvd[i, :, :PB].astype(F32)
        return 0

    lax.fori_loop(0, 2 * SIDE, collect, 0)

    for copy in started:
        copy.wait_send()
    for h in range(2):

        @pl.when(jnp.logical_not(own_block(h)))
        def _(h=h):
            for copy in gather(h):
                copy.wait_send()

    def drain(n, s):
        chain, across = onward(n, s)

        @pl.when(jnp.logical_not(last))
        def _():
            chain.wait_send()

        across.wait_send()

    for n in range(8):
        every_part(n, drain)

    def drain_diag(i, _):
        for s in range(2):
            copy = send(
                sendd.at[s, i], recvd.at[r], d_ssem.at[s, i], d_rsem.at[r],
                owner0 + i, SIDE * (y, twin)[s] + x,
            )
            if s:
                copy.wait_send()
            else:

                @pl.when(owner0 + i != r)
                def _(copy=copy):
                    copy.wait_send()

        return 0

    lax.fori_loop(0, SIDE, drain_diag, 0)


def inverted(struct_mask, ainv_anc, l_panel, diag_inv):
    rows, width = l_panel.shape
    vmem, dma = pltpu.VMEM, pltpu.SemaphoreType.DMA
    spec = pl.BlockSpec(memory_space=pltpu.VMEM)
    return pl.pallas_call(
        invert_kernel,
        out_shape=(
            jax.ShapeDtypeStruct((rows, width), BF16),
            jax.ShapeDtypeStruct(diag_inv.shape, F32),
        ),
        in_specs=[
            pl.BlockSpec(memory_space=pltpu.SMEM),
            pl.BlockSpec(memory_space=pl.ANY),
            spec,
            spec,
        ],
        out_specs=(spec, spec),
        scratch_shapes=[
            vmem((SIDE, 2, SUBS, SUB, HALF), BF16),
            vmem((SIDE * SIDE, SUBS, SUB, HALF), BF16),
            vmem(ainv_anc.shape, BF16),
            vmem((2, 4, 2, SIDE * PB, QUART), BF16),
            vmem((2, 6, SIDE * PB, QUART), BF16),
            vmem((2, SIDE, 2, PB, QUART), BF16),
            vmem((2, 6, PB, QUART), BF16),
            vmem((2, PB, HALF), BF16),
            vmem((2, PB, HALF), BF16),
            vmem((2, SIDE, PB, AB), BF16),
            vmem((2 * SIDE, PB, AB), BF16),
            dma(()),
            dma((6,)), dma((6,)),
            dma((2, SUBS)), dma((16, SUBS)),
            dma((8, SUBS)), dma((8, SUBS)), dma((16, SUBS)),
            dma((2, 6)), dma((2, 6)),
            dma((2, 6)), dma((2, 6)),
            dma((2,)), dma((2,)),
            dma((2, SIDE)), dma((2 * SIDE,)),
        ],
        compiler_params=pltpu.CompilerParams(
            collective_id=0, has_side_effects=True, vmem_limit_bytes=44 * 1024 * 1024
        ),
        cost_estimate=pl.CostEstimate(
            flops=100_000_000_000, bytes_accessed=12_000_000, transcendentals=0
        ),
        name="invert",
    )(struct_mask, ainv_anc, l_panel, diag_inv)


def local(ainv_anc, l_panel, diag_inv, struct_mask, pieces, tile_owner):
    devices = lax.axis_size("row") * lax.axis_size("col")
    slots = packed(tile_owner[:, 0], pieces, devices)
    parts = slots.reshape(devices, SLOT, *pieces.shape[1:])
    arrived = lax.all_to_all(parts, ("row", "col"), split_axis=0, concat_axis=0, tiled=True)
    upper, diag = inverted(struct_mask, ainv_anc, l_panel, diag_inv)
    moved = arrived.astype(F32).reshape(slots.shape)
    return upper, diag, moved


def solution(mesh):
    in_specs = (
        P("row", "col"),
        P("col", "row"),
        P("col", "row"),
        P(),
        P(("row", "col"), None, None),
        P(("row", "col"), None),
    )
    out_specs = (P("col", "row"), P("col", "row"), P(("row", "col"), None, None))
    return jax.shard_map(local, mesh=mesh, in_specs=in_specs, out_specs=out_specs, check_vma=False)
```

```python
import jax
import jax.numpy as jnp
from jax import lax
from jax.experimental import pallas as pl
from jax.experimental.pallas import tpu as pltpu
from jax.sharding import PartitionSpec as P

W = 768
AB = 128
SLOT = 3
SIDE = 4
PB = 96
SUBS, SUB = 3, 32
EVEN = ((2, 0), (2, 2), (0, 2), (0, 0), (1, 1), (1, 3), (3, 1), (3, 3))
ODD = ((2, 1), (2, 3), (1, 2), (3, 2), (1, 0), (3, 0), (0, 1), (0, 3))
HALF = 1536
QUART = 768
TILE = 256
BF16, F32 = jnp.bfloat16, jnp.float32


def pack_kernel(owner_ref, pieces_hbm, out_ref, pieces, count_ref, slot_ref, sems):
    parts = pieces.shape[0]
    per = pieces.shape[1]
    copies = [
        pltpu.make_async_copy(pieces_hbm.at[pl.ds(i * per, per)], pieces.at[i], sems.at[i])
        for i in range(parts)
    ]
    for copy in copies:
        copy.start()

    def reset(i, _):
        count_ref[i] = 0
        return 0

    lax.fori_loop(0, out_ref.shape[0] // SLOT, reset, 0, unroll=8)

    def number(p, _):
        owner = owner_ref[p]
        rank = count_ref[owner]
        count_ref[owner] = rank + 1
        slot_ref[p] = owner * SLOT + rank
        return 0

    lax.fori_loop(0, parts * per, number, 0, unroll=4)

    def clear(i, _):
        out_ref[pl.ds(i * 16, 16)] = jnp.zeros((16, *out_ref.shape[1:]), out_ref.dtype)
        return 0

    lax.fori_loop(0, out_ref.shape[0] // 16, clear, 0)

    for i in range(parts):
        copies[i].wait()

        def place(p, _, i=i):
            out_ref[slot_ref[i * per + p]] = pieces[i, p].astype(out_ref.dtype)
            return 0

        lax.fori_loop(0, per, place, 0, unroll=8)


def packed(owners, pieces, devices):
    count, *inside = pieces.shape
    parts = 4
    return pl.pallas_call(
        pack_kernel,
        out_shape=jax.ShapeDtypeStruct((devices * SLOT, *inside), BF16),
        in_specs=[
            pl.BlockSpec(memory_space=pltpu.SMEM),
            pl.BlockSpec(memory_space=pl.ANY),
        ],
        out_specs=pl.BlockSpec(memory_space=pltpu.VMEM),
        scratch_shapes=[
            pltpu.VMEM((parts, count // parts, *inside), pieces.dtype),
            pltpu.SMEM((devices,), jnp.int32),
            pltpu.SMEM((count,), jnp.int32),
            pltpu.SemaphoreType.DMA((parts,)),
        ],
        name="pack",
    )(owners, pieces)


def widen_kernel(narrow_hbm, wide_hbm, narrow, wide, in_sems, out_sems):
    parts, per = narrow.shape[:2]
    arriving = [
        pltpu.make_async_copy(narrow_hbm.at[pl.ds(i * per, per)], narrow.at[i], in_sems.at[i])
        for i in range(parts)
    ]
    leaving = [
        pltpu.make_async_copy(wide.at[i], wide_hbm.at[pl.ds(i * per, per)], out_sems.at[i])
        for i in range(parts)
    ]
    for copy in arriving:
        copy.start()
    for i in range(parts):
        arriving[i].wait()

        def cast(j, _, i=i):
            wide[i, pl.ds(j * 4, 4)] = narrow[i, pl.ds(j * 4, 4)].astype(F32)
            return 0

        lax.fori_loop(0, per // 4, cast, 0)
        leaving[i].start()
    for copy in leaving:
        copy.wait()


def widened(narrow):
    parts = 8
    inside = (parts, narrow.shape[0] // parts, *narrow.shape[1:])
    return pl.pallas_call(
        widen_kernel,
        out_shape=jax.ShapeDtypeStruct(narrow.shape, F32),
        in_specs=[pl.BlockSpec(memory_space=pl.ANY)],
        out_specs=pl.BlockSpec(memory_space=pl.ANY),
        scratch_shapes=[
            pltpu.VMEM(inside, narrow.dtype),
            pltpu.VMEM(inside, F32),
            pltpu.SemaphoreType.DMA((parts,)),
            pltpu.SemaphoreType.DMA((parts,)),
        ],
        name="widen",
    )(narrow)


def invert_kernel(
    mask_ref, a_hbm, panel_ref, dinv_ref, upper_ref, diag_ref,
    lmx, lm, a, part, in1, tot, in2, usend, ubuf, sendd, recvd,
    a_sem, x_ssem, x_rsem, g_ssem, l_rsem, c_ssem, f_ssem, f_rsem,
    p1_ssem, p1_rsem, p2_ssem, p2_rsem, u_ssem, u_rsem, d_ssem, d_rsem,
):
    r, c = lax.axis_index("row"), lax.axis_index("col")
    z, k = r // 2, r % 2
    y, x = c // SIDE, c % SIDE
    twin = y + 1 - 2 * (y % 2)
    node = c // (W // PB)
    started = []

    def at(row, col):
        return {"row": row, "col": col}

    def send(src, dst, ssem, rsem, row, col):
        return pltpu.make_async_remote_copy(
            src_ref=src, dst_ref=dst, send_sem=ssem, recv_sem=rsem,
            device_id=at(row, col), device_id_type=pl.DeviceIdType.MESH,
        )

    def go(*args):
        copy = send(*args)
        copy.start()
        started.append(copy)

    def arrived(dst, sem):
        send(dst, dst, sem, sem, r, c).wait_recv()

    a_copy = pltpu.make_async_copy(a_hbm, a, a_sem)
    a_copy.start()

    barrier = pltpu.get_barrier_semaphore()

    def greet(row, col):
        pl.semaphore_signal(
            barrier, inc=1, device_id=at(row, col), device_id_type=pl.DeviceIdType.MESH
        )

    def greet_plane(n, _):
        d = n // 2
        greet(2 * z + (k + n) % 2, SIDE * ((y + d // SIDE) % SIDE) + (x + d) % SIDE)
        return 0

    def greet_z(n, _):
        row = (2 * z + 2 + n) % (2 * SIDE)
        greet(row, c)
        greet(row, SIDE * twin + x)
        return 0

    lax.fori_loop(1, 2 * SIDE * SIDE, greet_plane, 0)
    lax.fori_loop(0, 2 * SIDE - 2, greet_z, 0)

    blocks = panel_ref.shape[1] // AB
    for b in range(blocks):
        keep = jnp.full((PB, AB), mask_ref[node, r * blocks + b], jnp.int32) > 0
        value = panel_ref[:, b * AB : (b + 1) * AB].astype(F32)
        h, o = divmod(b * AB, HALF)
        value = jnp.where(keep, value, 0.0).astype(BF16)
        lmx[x, h, :, :, o : o + AB] = value.reshape(SUBS, SUB, AB)

    pl.semaphore_wait(barrier, 2 * SIDE * SIDE - 1 + 2 * (2 * SIDE - 2))

    core = (x + y) % 2
    root_row = 2 * z + core

    def own_block(h):
        return (SIDE * z + 2 * k + h == c) & (k == core)

    def gather(h):
        return [
            send(
                lmx.at[x, h, s], lm.at[c, s], g_ssem.at[h, s], l_rsem.at[c, s],
                root_row, SIDE * z + 2 * k + h,
            )
            for s in range(SUBS)
        ]

    def soon(h):
        far_x = (x + SIDE - 2 * k - h) % SIDE == 2
        far_y = (y + SIDE - z) % SIDE == 2
        return far_x | far_y | (y == z)

    for h in range(2):

        @pl.when(own_block(h))
        def _(h=h):
            for s in range(SUBS):
                lm[c, s] = lmx[x, h, s]

        @pl.when(soon(h) & jnp.logical_not(own_block(h)))
        def _(h=h):
            for copy in gather(h):
                copy.start()

    xp, xm, xo = (x + 1) % SIDE, (x + 3) % SIDE, (x + 2) % SIDE
    right, left = SIDE * y + xp, SIDE * y + xm
    go(lmx.at[x, 0], lmx.at[x, 0], x_ssem.at[0], x_rsem.at[0], r, right)
    go(lmx.at[x, 1], lmx.at[x, 1], x_ssem.at[1], x_rsem.at[1], r, left)
    passed_on = (
        send(lmx.at[xm, 0], lmx.at[xm, 0], x_ssem.at[4], x_rsem.at[4], r, right),
        send(lmx.at[xp, 1], lmx.at[xp, 1], x_ssem.at[5], x_rsem.at[5], r, left),
    )
    started.extend(passed_on)

    def pass_on():
        arrived(lmx.at[xm, 0], x_rsem.at[0])
        passed_on[0].start()
        arrived(lmx.at[xp, 1], x_rsem.at[1])
        passed_on[1].start()

    @pl.when(y != z)
    def _():
        pass_on()
        for h in range(2):

            @pl.when(jnp.logical_not(soon(h)))
            def _(h=h):
                for copy in gather(h):
                    copy.start()

    other = 2 * z + 1 - k
    following = 2 * ((z + 1 + 2 * k) % SIDE) + k
    first, last = z == y, following // 2 == y

    def nth(n, mine):
        odd = (x + y + k + 1 - mine) % 2
        dx = EVEN[n][0] + odd * (ODD[n][0] - EVEN[n][0])
        dy = EVEN[n][1] + odd * (ODD[n][1] - EVEN[n][1])
        return SIDE * ((y + dy) % SIDE) + (x + dx) % SIDE

    def onward(n, s):
        b = nth(n, 1)
        return (
            send(lm.at[b, s], lm.at[b, s], c_ssem.at[n, s], l_rsem.at[b, s], following, c),
            send(lm.at[b, s], lm.at[b, s], f_ssem.at[n, s], f_rsem.at[b, s], other, c),
        )

    def hand_on(n, s):
        b = nth(n, 1)

        @pl.when(jnp.logical_not(first & (b == c) & (x // 2 == k)))
        def _():
            arrived(lm.at[b, s], l_rsem.at[b, s])

        chain, across = onward(n, s)

        @pl.when(jnp.logical_not(last))
        def _():
            chain.start()

        across.start()

    def every_part(n, act):
        def one(s, _):
            act(n, s)
            return 0

        lax.fori_loop(0, SUBS, one, 0)

    def take(n, s):
        b = nth(n, 0)
        arrived(lm.at[b, s], f_rsem.at[b, s])

    for n in range(4):
        every_part(n, hand_on)

    @pl.when(y == z)
    def _():
        pass_on()

    go(lmx.at[x, 1], lmx.at[x, 1], x_ssem.at[2], x_rsem.at[2], r, right)
    go(lmx.at[x, 0], lmx.at[x, 0], x_ssem.at[3], x_rsem.at[3], r, left)
    for n in range(4):
        every_part(n, take)
    a_copy.wait()

    place = (x, y)

    def neighbour(axis, step):
        if axis == 0:
            return r, SIDE * y + (x + step) % SIDE
        return r, SIDE * ((y + step) % SIDE) + x

    FAR, NEXT, LAST, OWN = range(4)

    def hop1(half, slot, piece, n, step):
        go(
            part.at[half, slot, piece], in1.at[half, n], p1_ssem.at[half, n], p1_rsem.at[half, n],
            *neighbour(half, step),
        )

    def multiply(half, slot, dest, blocks_due=()):
        across, along = (SIDE, 1) if half == 0 else (1, SIDE)

        def tile(t, _):
            rows = jnp.concatenate(
                [lm[j * across + dest * along].reshape(PB, HALF) for j in range(SIDE)], axis=0
            )
            cols = a[pl.ds(pl.multiple_of(half * HALF + t * TILE, TILE), TILE), :]
            value = lax.dot_general(rows, cols, (((1,), (1,)), ((), ())), preferred_element_type=F32)
            per = QUART // TILE
            part[half, slot, t // per, :, pl.ds(pl.multiple_of((t % per) * TILE, TILE), TILE)] = value.astype(BF16)
            return 0

        if not blocks_due:
            lax.fori_loop(0, HALF // TILE, tile, 0)
        for i, n in enumerate(blocks_due):

            def tile_and_part(s, _, i=i, n=n):
                tile(SUBS * i + s, 0)
                hand_on(n, s)
                return 0

            lax.fori_loop(0, SUBS, tile_and_part, 0)
            hop1(half, slot, i, i, 1 + 2 * i)

    def add1(half, slot, piece, n):
        arrived(in1.at[half, n], p1_rsem.at[half, n])

        def rows(i, _):
            s = pl.ds(pl.multiple_of(i * 32, 32), 32)
            value = part[half, slot, piece, s, :].astype(F32) + in1[half, n, s, :].astype(F32)
            part[half, slot, piece, s, :] = value.astype(BF16)
            return 0

        lax.fori_loop(0, SIDE * PB // 32, rows, 0)

    for half in range(2):
        multiply(half, FAR, (place[half] + 2) % SIDE, (4 + 2 * half, 5 + 2 * half))
    for n in range(4, 8):
        every_part(n, take)
    for half in range(2):
        multiply(half, NEXT, (place[half] + 1) % SIDE)
        hop1(half, NEXT, 1, 3, 1)
        multiply(half, LAST, (place[half] + 3) % SIDE)
        hop1(half, LAST, 0, 5, 3)
    for half in range(2):
        add1(half, NEXT, 0, 0)
        hop1(half, NEXT, 0, 2, 1)
        add1(half, LAST, 1, 1)
        hop1(half, LAST, 1, 4, 3)
    for half in range(2):
        multiply(half, OWN, place[half])

    def hop2(half, group, piece, n, step):
        go(
            tot.at[half, group, piece], in2.at[half, n], p2_ssem.at[half, n], p2_rsem.at[half, n],
            *neighbour(1 - half, step),
        )

    def add2(half, group, piece, n):
        arrived(in2.at[half, n], p2_rsem.at[half, n])
        value = tot[half, group, piece].astype(F32) + in2[half, n].astype(F32)
        tot[half, group, piece] = value.astype(BF16)

    for half in range(2):
        q = place[1 - half]
        for n in (3, 5, 2, 4):
            arrived(in1.at[half, n], p1_rsem.at[half, n])

        def sums(i, _, half=half):
            s = pl.ds(pl.multiple_of(i * PB, PB), PB)
            for piece, (m, n) in enumerate(((2, 5), (3, 4))):
                value = part[half, OWN, piece, s, :].astype(F32) + in1[half, m, s, :].astype(F32)
                tot[half, i, piece] = (value + in1[half, n, s, :].astype(F32)).astype(BF16)
            return 0

        lax.fori_loop(0, SIDE, sums, 0)
        hop2(half, (q + 2) % SIDE, 0, 0, 1)
        hop2(half, (q + 2) % SIDE, 1, 1, 3)
        hop2(half, (q + 1) % SIDE, 1, 3, 1)
        hop2(half, (q + 3) % SIDE, 0, 5, 3)
    for half in range(2):
        q = place[1 - half]
        add2(half, (q + 1) % SIDE, 0, 0)
        hop2(half, (q + 1) % SIDE, 0, 2, 1)
        add2(half, (q + 3) % SIDE, 1, 1)
        hop2(half, (q + 3) % SIDE, 1, 4, 3)

    for half in range(2):
        q = place[1 - half]
        for n in (3, 5, 2, 4):
            arrived(in2.at[half, n], p2_rsem.at[half, n])
        for piece, (m, n) in enumerate(((2, 5), (3, 4))):
            for b in range(QUART // AB):
                s = slice(b * AB, (b + 1) * AB)
                o = piece * QUART + b * AB
                keep = mask_ref[node, r * blocks + (half * HALF + o) // AB]
                value = tot[half, q, piece, :, s].astype(F32) + in2[half, m, :, s].astype(F32)
                value = value + in2[half, n, :, s].astype(F32)
                value = jnp.where(jnp.full((PB, AB), keep, jnp.int32) > 0, -value, 0.0).astype(BF16)
                upper_ref[:, half * HALF + o : half * HALF + o + AB] = value
                usend[half, :, o : o + AB] = value
        go(usend.at[half], ubuf.at[half], u_ssem.at[half], u_rsem.at[half], r, SIDE * twin + x)

    for n, (b, h) in enumerate(((xm, 1), (xp, 0), (xo, 0), (xo, 1))):
        arrived(lmx.at[b, h], x_rsem.at[2 + n])

    owner0 = (y % 2) * SIDE

    def partial(s, source):
        def one(i, _):
            value = jnp.zeros((PB, PB), F32)
            for h in range(2):
                value = value + lax.dot_general(
                    source[h], lmx[i, h].reshape(PB, HALF), (((1,), (1,)), ((), ())),
                    preferred_element_type=F32,
                )
            sendd[s, i, :, :PB] = value.astype(BF16)
            copy = send(
                sendd.at[s, i], recvd.at[r], d_ssem.at[s, i], d_rsem.at[r],
                owner0 + i, SIDE * (y, twin)[s] + x,
            )
            if s:
                copy.start()
            else:

                @pl.when(owner0 + i == r)
                def _():
                    recvd[r] = sendd[s, i]

                @pl.when(owner0 + i != r)
                def _():
                    copy.start()

            return 0

        lax.fori_loop(0, SIDE, one, 0)

    sendd[...] = jnp.zeros_like(sendd)
    partial(0, usend)
    for h in range(2):
        arrived(ubuf.at[h], u_rsem.at[h])
    partial(1, ubuf)

    diag_ref[...] = dinv_ref[...]

    def collect(i, _):
        @pl.when(jnp.logical_not((i == r) & (r // SIDE == y % 2)))
        def _():
            arrived(recvd.at[i], d_rsem.at[i])

        diag_ref[...] = diag_ref[...] - recvd[i, :, :PB].astype(F32)
        return 0

    lax.fori_loop(0, 2 * SIDE, collect, 0)

    for copy in started:
        copy.wait_send()
    for h in range(2):

        @pl.when(jnp.logical_not(own_block(h)))
        def _(h=h):
            for copy in gather(h):
                copy.wait_send()

    def drain(n, s):
        chain, across = onward(n, s)

        @pl.when(jnp.logical_not(last))
        def _():
            chain.wait_send()

        across.wait_send()

    for n in range(8):
        every_part(n, drain)

    def drain_diag(i, _):
        for s in range(2):
            copy = send(
                sendd.at[s, i], recvd.at[r], d_ssem.at[s, i], d_rsem.at[r],
                owner0 + i, SIDE * (y, twin)[s] + x,
            )
            if s:
                copy.wait_send()
            else:

                @pl.when(owner0 + i != r)
                def _(copy=copy):
                    copy.wait_send()

        return 0

    lax.fori_loop(0, SIDE, drain_diag, 0)


def inverted(struct_mask, ainv_anc, l_panel, diag_inv):
    rows, width = l_panel.shape
    vmem, dma = pltpu.VMEM, pltpu.SemaphoreType.DMA
    spec = pl.BlockSpec(memory_space=pltpu.VMEM)
    return pl.pallas_call(
        invert_kernel,
        out_shape=(
            jax.ShapeDtypeStruct((rows, width), BF16),
            jax.ShapeDtypeStruct(diag_inv.shape, F32),
        ),
        in_specs=[
            pl.BlockSpec(memory_space=pltpu.SMEM),
            pl.BlockSpec(memory_space=pl.ANY),
            spec,
            spec,
        ],
        out_specs=(spec, spec),
        scratch_shapes=[
            vmem((SIDE, 2, SUBS, SUB, HALF), BF16),
            vmem((SIDE * SIDE, SUBS, SUB, HALF), BF16),
            vmem(ainv_anc.shape, BF16),
            vmem((2, 4, 2, SIDE * PB, QUART), BF16),
            vmem((2, 6, SIDE * PB, QUART), BF16),
            vmem((2, SIDE, 2, PB, QUART), BF16),
            vmem((2, 6, PB, QUART), BF16),
            vmem((2, PB, HALF), BF16),
            vmem((2, PB, HALF), BF16),
            vmem((2, SIDE, PB, AB), BF16),
            vmem((2 * SIDE, PB, AB), BF16),
            dma(()),
            dma((6,)), dma((6,)),
            dma((2, SUBS)), dma((16, SUBS)),
            dma((8, SUBS)), dma((8, SUBS)), dma((16, SUBS)),
            dma((2, 6)), dma((2, 6)),
            dma((2, 6)), dma((2, 6)),
            dma((2,)), dma((2,)),
            dma((2, SIDE)), dma((2 * SIDE,)),
        ],
        compiler_params=pltpu.CompilerParams(
            collective_id=0, has_side_effects=True, vmem_limit_bytes=44 * 1024 * 1024
        ),
        cost_estimate=pl.CostEstimate(
            flops=100_000_000_000, bytes_accessed=12_000_000, transcendentals=0
        ),
        name="invert",
    )(struct_mask, ainv_anc, l_panel, diag_inv)


def local(ainv_anc, l_panel, diag_inv, struct_mask, pieces, tile_owner):
    devices = lax.axis_size("row") * lax.axis_size("col")
    slots = packed(tile_owner[:, 0], pieces, devices)
    parts = slots.reshape(devices, SLOT, *pieces.shape[1:])
    arrived = lax.all_to_all(parts, ("row", "col"), split_axis=0, concat_axis=0, tiled=True)
    upper, diag = inverted(struct_mask, ainv_anc, l_panel, diag_inv)
    moved = widened(arrived.reshape(slots.shape))
    return upper, diag, moved


def solution(mesh):
    in_specs = (
        P("row", "col"),
        P("col", "row"),
        P("col", "row"),
        P(),
        P(("row", "col"), None, None),
        P(("row", "col"), None),
    )
    out_specs = (P("col", "row"), P("col", "row"), P(("row", "col"), None, None))
    return jax.shard_map(local, mesh=mesh, in_specs=in_specs, out_specs=out_specs, check_vma=False)
```

```python
import jax
import jax.numpy as jnp
from jax import lax
from jax.experimental import pallas as pl
from jax.experimental.pallas import tpu as pltpu
from jax.sharding import PartitionSpec as P

W = 768
AB = 128
SLOT = 3
SIDE = 4
PB = 96
SUBS, SUB = 3, 32
EVEN = ((2, 0), (2, 2), (0, 2), (0, 0), (1, 1), (1, 3), (3, 1), (3, 3))
ODD = ((2, 1), (2, 3), (1, 2), (3, 2), (1, 0), (3, 0), (0, 1), (0, 3))
HALF = 1536
QUART = 768
TILE = 256
BF16, F32 = jnp.bfloat16, jnp.float32


def pack_kernel(owner_ref, pieces_hbm, out_ref, pieces, count_ref, slot_ref, sems):
    parts = pieces.shape[0]
    per = pieces.shape[1]
    copies = [
        pltpu.make_async_copy(pieces_hbm.at[pl.ds(i * per, per)], pieces.at[i], sems.at[i])
        for i in range(parts)
    ]
    for copy in copies:
        copy.start()

    def reset(i, _):
        count_ref[i] = 0
        return 0

    lax.fori_loop(0, out_ref.shape[0] // SLOT, reset, 0, unroll=8)

    def number(p, _):
        owner = owner_ref[p]
        rank = count_ref[owner]
        count_ref[owner] = rank + 1
        slot_ref[p] = owner * SLOT + rank
        return 0

    lax.fori_loop(0, parts * per, number, 0, unroll=4)

    def clear(i, _):
        out_ref[pl.ds(i * 16, 16)] = jnp.zeros((16, *out_ref.shape[1:]), out_ref.dtype)
        return 0

    lax.fori_loop(0, out_ref.shape[0] // 16, clear, 0)

    for i in range(parts):
        copies[i].wait()

        def place(p, _, i=i):
            out_ref[slot_ref[i * per + p]] = pieces[i, p].astype(out_ref.dtype)
            return 0

        lax.fori_loop(0, per, place, 0, unroll=8)


def packed(owners, pieces, devices):
    count, *inside = pieces.shape
    parts = 4
    return pl.pallas_call(
        pack_kernel,
        out_shape=jax.ShapeDtypeStruct((devices * SLOT, *inside), BF16),
        in_specs=[
            pl.BlockSpec(memory_space=pltpu.SMEM),
            pl.BlockSpec(memory_space=pl.ANY),
        ],
        out_specs=pl.BlockSpec(memory_space=pltpu.VMEM),
        scratch_shapes=[
            pltpu.VMEM((parts, count // parts, *inside), pieces.dtype),
            pltpu.SMEM((devices,), jnp.int32),
            pltpu.SMEM((count,), jnp.int32),
            pltpu.SemaphoreType.DMA((parts,)),
        ],
        name="pack",
    )(owners, pieces)


def widen_kernel(narrow_hbm, wide_hbm, narrow, wide, in_sems, out_sems):
    parts, per = narrow.shape[:2]
    arriving = [
        pltpu.make_async_copy(narrow_hbm.at[pl.ds(i * per, per)], narrow.at[i], in_sems.at[i])
        for i in range(parts)
    ]
    leaving = [
        pltpu.make_async_copy(wide.at[i], wide_hbm.at[pl.ds(i * per, per)], out_sems.at[i])
        for i in range(parts)
    ]
    for copy in arriving:
        copy.start()
    for i in range(parts):
        arriving[i].wait()

        def cast(j, _, i=i):
            wide[i, pl.ds(j * 4, 4)] = narrow[i, pl.ds(j * 4, 4)].astype(F32)
            return 0

        lax.fori_loop(0, per // 4, cast, 0)
        leaving[i].start()
    for copy in leaving:
        copy.wait()


def widened(narrow):
    parts = 8
    inside = (parts, narrow.shape[0] // parts, *narrow.shape[1:])
    return pl.pallas_call(
        widen_kernel,
        out_shape=jax.ShapeDtypeStruct(narrow.shape, F32),
        in_specs=[pl.BlockSpec(memory_space=pl.ANY)],
        out_specs=pl.BlockSpec(memory_space=pl.ANY),
        scratch_shapes=[
            pltpu.VMEM(inside, narrow.dtype),
            pltpu.VMEM(inside, F32),
            pltpu.SemaphoreType.DMA((parts,)),
            pltpu.SemaphoreType.DMA((parts,)),
        ],
        name="widen",
    )(narrow)


def invert_kernel(
    mask_ref, a_hbm, panel_ref, dinv_ref, upper_ref, diag_ref,
    lmx, lm, a, part, in1, tot, in2, usend, ubuf, sendd, recvd,
    a_sem, x_ssem, x_rsem, g_ssem, l_rsem, c_ssem, f_ssem, f_rsem,
    p1_ssem, p1_rsem, p2_ssem, p2_rsem, u_ssem, u_rsem, d_ssem, d_rsem,
):
    r, c = lax.axis_index("row"), lax.axis_index("col")
    z, k = r // 2, r % 2
    y, x = c // SIDE, c % SIDE
    twin = y + 1 - 2 * (y % 2)
    node = c // (W // PB)
    started = []

    def at(row, col):
        return {"row": row, "col": col}

    def send(src, dst, ssem, rsem, row, col):
        return pltpu.make_async_remote_copy(
            src_ref=src, dst_ref=dst, send_sem=ssem, recv_sem=rsem,
            device_id=at(row, col), device_id_type=pl.DeviceIdType.MESH,
        )

    def go(*args):
        copy = send(*args)
        copy.start()
        started.append(copy)

    def arrived(dst, sem):
        send(dst, dst, sem, sem, r, c).wait_recv()

    a_copy = pltpu.make_async_copy(a_hbm, a, a_sem)
    a_copy.start()

    barrier = pltpu.get_barrier_semaphore()

    def greet(row, col):
        pl.semaphore_signal(
            barrier, inc=1, device_id=at(row, col), device_id_type=pl.DeviceIdType.MESH
        )

    def greet_plane(n, _):
        d = n // 2
        greet(2 * z + (k + n) % 2, SIDE * ((y + d // SIDE) % SIDE) + (x + d) % SIDE)
        return 0

    def greet_z(n, _):
        row = (2 * z + 2 + n) % (2 * SIDE)
        greet(row, c)
        greet(row, SIDE * twin + x)
        return 0

    lax.fori_loop(1, 2 * SIDE * SIDE, greet_plane, 0)
    lax.fori_loop(0, 2 * SIDE - 2, greet_z, 0)

    blocks = panel_ref.shape[1] // AB
    for b in range(blocks):
        keep = jnp.full((PB, AB), mask_ref[node, r * blocks + b], jnp.int32) > 0
        value = panel_ref[:, b * AB : (b + 1) * AB].astype(F32)
        h, o = divmod(b * AB, HALF)
        value = jnp.where(keep, value, 0.0).astype(BF16)
        lmx[x, h, :, :, o : o + AB] = value.reshape(SUBS, SUB, AB)

    pl.semaphore_wait(barrier, 2 * SIDE * SIDE - 1 + 2 * (2 * SIDE - 2))

    core = (x + y) % 2
    root_row = 2 * z + core

    def own_block(h):
        return (SIDE * z + 2 * k + h == c) & (k == core)

    def gather(h):
        return [
            send(
                lmx.at[x, h, s], lm.at[c, s], g_ssem.at[h, s], l_rsem.at[c, s],
                root_row, SIDE * z + 2 * k + h,
            )
            for s in range(SUBS)
        ]

    def soon(h):
        far_x = (x + SIDE - 2 * k - h) % SIDE == 2
        far_y = (y + SIDE - z) % SIDE == 2
        return far_x | far_y | (y == z)

    for h in range(2):

        @pl.when(own_block(h))
        def _(h=h):
            for s in range(SUBS):
                lm[c, s] = lmx[x, h, s]

        @pl.when(soon(h) & jnp.logical_not(own_block(h)))
        def _(h=h):
            for copy in gather(h):
                copy.start()

    xp, xm, xo = (x + 1) % SIDE, (x + 3) % SIDE, (x + 2) % SIDE
    right, left = SIDE * y + xp, SIDE * y + xm
    go(lmx.at[x, 0], lmx.at[x, 0], x_ssem.at[0], x_rsem.at[0], r, right)
    go(lmx.at[x, 1], lmx.at[x, 1], x_ssem.at[1], x_rsem.at[1], r, left)
    passed_on = (
        send(lmx.at[xm, 0], lmx.at[xm, 0], x_ssem.at[4], x_rsem.at[4], r, right),
        send(lmx.at[xp, 1], lmx.at[xp, 1], x_ssem.at[5], x_rsem.at[5], r, left),
    )
    started.extend(passed_on)

    def pass_on():
        arrived(lmx.at[xm, 0], x_rsem.at[0])
        passed_on[0].start()
        arrived(lmx.at[xp, 1], x_rsem.at[1])
        passed_on[1].start()

    @pl.when(y != z)
    def _():
        pass_on()
        for h in range(2):

            @pl.when(jnp.logical_not(soon(h)))
            def _(h=h):
                for copy in gather(h):
                    copy.start()

    other = 2 * z + 1 - k
    following = 2 * ((z + 1 + 2 * k) % SIDE) + k
    first, last = z == y, following // 2 == y

    def nth(n, mine):
        odd = (x + y + k + 1 - mine) % 2
        dx = EVEN[n][0] + odd * (ODD[n][0] - EVEN[n][0])
        dy = EVEN[n][1] + odd * (ODD[n][1] - EVEN[n][1])
        return SIDE * ((y + dy) % SIDE) + (x + dx) % SIDE

    def onward(n, s):
        b = nth(n, 1)
        return (
            send(lm.at[b, s], lm.at[b, s], c_ssem.at[n, s], l_rsem.at[b, s], following, c),
            send(lm.at[b, s], lm.at[b, s], f_ssem.at[n, s], f_rsem.at[b, s], other, c),
        )

    def hand_on(n, s):
        b = nth(n, 1)

        @pl.when(jnp.logical_not(first & (b == c) & (x // 2 == k)))
        def _():
            arrived(lm.at[b, s], l_rsem.at[b, s])

        chain, across = onward(n, s)

        @pl.when(jnp.logical_not(last))
        def _():
            chain.start()

        across.start()

    def every_part(n, act):
        def one(s, _):
            act(n, s)
            return 0

        lax.fori_loop(0, SUBS, one, 0)

    def take(n, s):
        b = nth(n, 0)
        arrived(lm.at[b, s], f_rsem.at[b, s])

    for n in range(4):
        every_part(n, hand_on)

    @pl.when(y == z)
    def _():
        pass_on()

    go(lmx.at[x, 1], lmx.at[x, 1], x_ssem.at[2], x_rsem.at[2], r, right)
    go(lmx.at[x, 0], lmx.at[x, 0], x_ssem.at[3], x_rsem.at[3], r, left)
    for n in range(4):
        every_part(n, take)
    a_copy.wait()

    place = (x, y)

    def neighbour(axis, step):
        if axis == 0:
            return r, SIDE * y + (x + step) % SIDE
        return r, SIDE * ((y + step) % SIDE) + x

    FAR, NEXT, LAST, OWN = range(4)

    def hop1(half, slot, piece, n, step):
        go(
            part.at[half, slot, piece], in1.at[half, n], p1_ssem.at[half, n], p1_rsem.at[half, n],
            *neighbour(half, step),
        )

    def multiply(half, slot, dest, blocks_due=(), direct=None):
        across, along = (SIDE, 1) if half == 0 else (1, SIDE)

        def tile(t, _):
            rows = jnp.concatenate(
                [lm[j * across + dest * along].reshape(PB, HALF) for j in range(SIDE)], axis=0
            )
            cols = a[pl.ds(pl.multiple_of(half * HALF + t * TILE, TILE), TILE), :]
            value = lax.dot_general(rows, cols, (((1,), (1,)), ((), ())), preferred_element_type=F32)
            per = QUART // TILE
            part[half, slot, t // per, :, pl.ds(pl.multiple_of((t % per) * TILE, TILE), TILE)] = value.astype(BF16)
            return 0

        per = QUART // TILE
        if direct is not None:
            piece, n, step = direct
            lax.fori_loop(piece * per, (piece + 1) * per, tile, 0)
            hop1(half, slot, piece, n, step)
            lax.fori_loop((1 - piece) * per, (2 - piece) * per, tile, 0)
        elif not blocks_due:
            lax.fori_loop(0, HALF // TILE, tile, 0)
        for i, n in enumerate(blocks_due):

            def tile_and_part(s, _, i=i, n=n):
                tile(SUBS * i + s, 0)
                hand_on(n, s)
                return 0

            lax.fori_loop(0, SUBS, tile_and_part, 0)
            hop1(half, slot, i, i, 1 + 2 * i)

    def add1(half, slot, piece, n):
        arrived(in1.at[half, n], p1_rsem.at[half, n])

        def rows(i, _):
            s = pl.ds(pl.multiple_of(i * 32, 32), 32)
            value = part[half, slot, piece, s, :].astype(F32) + in1[half, n, s, :].astype(F32)
            part[half, slot, piece, s, :] = value.astype(BF16)
            return 0

        lax.fori_loop(0, SIDE * PB // 32, rows, 0)

    for half in range(2):
        multiply(half, FAR, (place[half] + 2) % SIDE, (4 + 2 * half, 5 + 2 * half))
    for n in range(4, 8):
        every_part(n, take)
    for half in range(2):
        multiply(half, NEXT, (place[half] + 1) % SIDE, direct=(1, 3, 1))
        multiply(half, LAST, (place[half] + 3) % SIDE, direct=(0, 5, 3))
    for half in range(2):
        add1(half, NEXT, 0, 0)
        hop1(half, NEXT, 0, 2, 1)
        add1(half, LAST, 1, 1)
        hop1(half, LAST, 1, 4, 3)
    for half in range(2):
        multiply(half, OWN, place[half])

    def hop2(half, group, piece, n, step):
        go(
            tot.at[half, group, piece], in2.at[half, n], p2_ssem.at[half, n], p2_rsem.at[half, n],
            *neighbour(1 - half, step),
        )

    def add2(half, group, piece, n):
        arrived(in2.at[half, n], p2_rsem.at[half, n])
        value = tot[half, group, piece].astype(F32) + in2[half, n].astype(F32)
        tot[half, group, piece] = value.astype(BF16)

    for half in range(2):
        q = place[1 - half]
        for n in (3, 5, 2, 4):
            arrived(in1.at[half, n], p1_rsem.at[half, n])

        def sums(i, _, half=half):
            s = pl.ds(pl.multiple_of(i * PB, PB), PB)
            for piece, (m, n) in enumerate(((2, 5), (3, 4))):
                value = part[half, OWN, piece, s, :].astype(F32) + in1[half, m, s, :].astype(F32)
                tot[half, i, piece] = (value + in1[half, n, s, :].astype(F32)).astype(BF16)
            return 0

        lax.fori_loop(0, SIDE, sums, 0)
        hop2(half, (q + 2) % SIDE, 0, 0, 1)
        hop2(half, (q + 2) % SIDE, 1, 1, 3)
        hop2(half, (q + 1) % SIDE, 1, 3, 1)
        hop2(half, (q + 3) % SIDE, 0, 5, 3)
    for half in range(2):
        q = place[1 - half]
        add2(half, (q + 1) % SIDE, 0, 0)
        hop2(half, (q + 1) % SIDE, 0, 2, 1)
        add2(half, (q + 3) % SIDE, 1, 1)
        hop2(half, (q + 3) % SIDE, 1, 4, 3)

    for half in range(2):
        q = place[1 - half]
        for n in (3, 5, 2, 4):
            arrived(in2.at[half, n], p2_rsem.at[half, n])
        for piece, (m, n) in enumerate(((2, 5), (3, 4))):
            for b in range(QUART // AB):
                s = slice(b * AB, (b + 1) * AB)
                o = piece * QUART + b * AB
                keep = mask_ref[node, r * blocks + (half * HALF + o) // AB]
                value = tot[half, q, piece, :, s].astype(F32) + in2[half, m, :, s].astype(F32)
                value = value + in2[half, n, :, s].astype(F32)
                value = jnp.where(jnp.full((PB, AB), keep, jnp.int32) > 0, -value, 0.0).astype(BF16)
                upper_ref[:, half * HALF + o : half * HALF + o + AB] = value
                usend[half, :, o : o + AB] = value
        go(usend.at[half], ubuf.at[half], u_ssem.at[half], u_rsem.at[half], r, SIDE * twin + x)

    for n, (b, h) in enumerate(((xm, 1), (xp, 0), (xo, 0), (xo, 1))):
        arrived(lmx.at[b, h], x_rsem.at[2 + n])

    owner0 = (y % 2) * SIDE

    def partial(s, source):
        def one(i, _):
            value = jnp.zeros((PB, PB), F32)
            for h in range(2):
                value = value + lax.dot_general(
                    source[h], lmx[i, h].reshape(PB, HALF), (((1,), (1,)), ((), ())),
                    preferred_element_type=F32,
                )
            sendd[s, i, :, :PB] = value.astype(BF16)
            copy = send(
                sendd.at[s, i], recvd.at[r], d_ssem.at[s, i], d_rsem.at[r],
                owner0 + i, SIDE * (y, twin)[s] + x,
            )
            if s:
                copy.start()
            else:

                @pl.when(owner0 + i == r)
                def _():
                    recvd[r] = sendd[s, i]

                @pl.when(owner0 + i != r)
                def _():
                    copy.start()

            return 0

        lax.fori_loop(0, SIDE, one, 0)

    sendd[...] = jnp.zeros_like(sendd)
    partial(0, usend)
    for h in range(2):
        arrived(ubuf.at[h], u_rsem.at[h])
    partial(1, ubuf)

    diag_ref[...] = dinv_ref[...]

    def collect(i, _):
        @pl.when(jnp.logical_not((i == r) & (r // SIDE == y % 2)))
        def _():
            arrived(recvd.at[i], d_rsem.at[i])

        diag_ref[...] = diag_ref[...] - recvd[i, :, :PB].astype(F32)
        return 0

    lax.fori_loop(0, 2 * SIDE, collect, 0)

    for copy in started:
        copy.wait_send()
    for h in range(2):

        @pl.when(jnp.logical_not(own_block(h)))
        def _(h=h):
            for copy in gather(h):
                copy.wait_send()

    def drain(n, s):
        chain, across = onward(n, s)

        @pl.when(jnp.logical_not(last))
        def _():
            chain.wait_send()

        across.wait_send()

    for n in range(8):
        every_part(n, drain)

    def drain_diag(i, _):
        for s in range(2):
            copy = send(
                sendd.at[s, i], recvd.at[r], d_ssem.at[s, i], d_rsem.at[r],
                owner0 + i, SIDE * (y, twin)[s] + x,
            )
            if s:
                copy.wait_send()
            else:

                @pl.when(owner0 + i != r)
                def _(copy=copy):
                    copy.wait_send()

        return 0

    lax.fori_loop(0, SIDE, drain_diag, 0)


def inverted(struct_mask, ainv_anc, l_panel, diag_inv):
    rows, width = l_panel.shape
    vmem, dma = pltpu.VMEM, pltpu.SemaphoreType.DMA
    spec = pl.BlockSpec(memory_space=pltpu.VMEM)
    return pl.pallas_call(
        invert_kernel,
        out_shape=(
            jax.ShapeDtypeStruct((rows, width), BF16),
            jax.ShapeDtypeStruct(diag_inv.shape, F32),
        ),
        in_specs=[
            pl.BlockSpec(memory_space=pltpu.SMEM),
            pl.BlockSpec(memory_space=pl.ANY),
            spec,
            spec,
        ],
        out_specs=(spec, spec),
        scratch_shapes=[
            vmem((SIDE, 2, SUBS, SUB, HALF), BF16),
            vmem((SIDE * SIDE, SUBS, SUB, HALF), BF16),
            vmem(ainv_anc.shape, BF16),
            vmem((2, 4, 2, SIDE * PB, QUART), BF16),
            vmem((2, 6, SIDE * PB, QUART), BF16),
            vmem((2, SIDE, 2, PB, QUART), BF16),
            vmem((2, 6, PB, QUART), BF16),
            vmem((2, PB, HALF), BF16),
            vmem((2, PB, HALF), BF16),
            vmem((2, SIDE, PB, AB), BF16),
            vmem((2 * SIDE, PB, AB), BF16),
            dma(()),
            dma((6,)), dma((6,)),
            dma((2, SUBS)), dma((16, SUBS)),
            dma((8, SUBS)), dma((8, SUBS)), dma((16, SUBS)),
            dma((2, 6)), dma((2, 6)),
            dma((2, 6)), dma((2, 6)),
            dma((2,)), dma((2,)),
            dma((2, SIDE)), dma((2 * SIDE,)),
        ],
        compiler_params=pltpu.CompilerParams(
            collective_id=0, has_side_effects=True, vmem_limit_bytes=44 * 1024 * 1024
        ),
        cost_estimate=pl.CostEstimate(
            flops=100_000_000_000, bytes_accessed=12_000_000, transcendentals=0
        ),
        name="invert",
    )(struct_mask, ainv_anc, l_panel, diag_inv)


def local(ainv_anc, l_panel, diag_inv, struct_mask, pieces, tile_owner):
    devices = lax.axis_size("row") * lax.axis_size("col")
    slots = packed(tile_owner[:, 0], pieces, devices)
    parts = slots.reshape(devices, SLOT, *pieces.shape[1:])
    arrived = lax.all_to_all(parts, ("row", "col"), split_axis=0, concat_axis=0, tiled=True)
    upper, diag = inverted(struct_mask, ainv_anc, l_panel, diag_inv)
    moved = widened(arrived.reshape(slots.shape))
    return upper, diag, moved


def solution(mesh):
    in_specs = (
        P("row", "col"),
        P("col", "row"),
        P("col", "row"),
        P(),
        P(("row", "col"), None, None),
        P(("row", "col"), None),
    )
    out_specs = (P("col", "row"), P("col", "row"), P(("row", "col"), None, None))
    return jax.shard_map(local, mesh=mesh, in_specs=in_specs, out_specs=out_specs, check_vma=False)
```
